256 devices in a mesh: row: 16 (over z, core), col: 4 (over x), depth: 4 (over y).
Axes of the slice: x: 4, y: 4, z: 8, core: 2. Of those that a mesh axis runs over, the one named last changes fastest.
Arguments:
- diag_block: float32 [512, 512], P(('row', 'col')), may hold values from -40 to 60, as said below
- panel: float32 [16384, 512], P(('row', 'col'), 'depth'), may hold values from -1.2 to 1.2
- trailing: float32 [16384, 16384], P(('col', 'depth'), 'row'), may hold values from -6 to 6
Outputs:
- factor_diag: float32 [512, 512], P(('row', 'col'))
- factor_panel: float32 [16384, 512], P(('row', 'col'), 'depth')
- schur: float32 [16384, 16384], P(('col', 'depth'), 'row')
The draws below stay inside these ranges and needn't reach their ends.
Inputs may be any that keep to these rules, and one draw needn't show every extreme that they name: `diag_block`: symmetric, with every eigenvalue 1 or more.
All inputs are finite; a program needn't handle non-finite values.
Results may differ from the reference program's by a relative error of at most 0.000071.
Values sent between devices are 32-bit elements; how exact they have to be, the bound alone decides.
A program may use at most 128 MiB of HBM per device.

```python
import jax
import jax.numpy as jnp
from jax import lax

TRAIL = 16384
BLOCK = 512


def draw_diag_block(key, part):
    base = jax.random.normal(jax.random.fold_in(key, 11), (BLOCK, BLOCK), jnp.float32)
    gram = jnp.dot(base, base.T, precision=lax.Precision.HIGHEST) / BLOCK
    result = 0.5 * (gram + gram.T) + jnp.eye(BLOCK, dtype=jnp.float32)
    return result


def levels(stream_key, shape, cuts, smallest, top_value):
    gain = 1.0
    for dim, parts in cuts:
        heights = jax.random.uniform(jax.random.fold_in(jax.random.fold_in(stream_key, 6), dim), (parts,), jnp.float32, smallest / len(cuts), top_value / len(cuts))
        gain = gain * jnp.repeat(jnp.exp(heights), shape[dim] // parts).reshape((-1,) + (1,) * (len(shape) - 1 - dim))
    return gain


def centred(key, extent, width, limit, cuts=(), kind=jnp.bfloat16):
    values = width * jax.random.normal(key, extent, jnp.float32)
    if cuts:
        values = values * levels(key, extent, cuts, -0.22, 0.18)
    return jnp.clip(values, -limit, limit).astype(kind)


def setup_inputs(seed: int = 0) -> dict:
    keys = jax.random.split(jax.random.key(seed), 4)
    return {
        "diag_block": draw_diag_block(jax.random.fold_in(keys[3], 71), 0),
        "panel": centred(keys[1], (TRAIL, BLOCK), 0.2, 1.2, ((0, 64), (1, 4)), jnp.float32),
        "trailing": centred(keys[2], (TRAIL, TRAIL), 1.0, 6.0, ((0, 16), (1, 16)), jnp.float32),
    }


def outer_rows(left, right):
    return lax.dot_general(left.astype(jnp.float32), right.astype(jnp.float32), (((1,), (1,)), ((), ())), precision=lax.Precision.HIGHEST, preferred_element_type=jnp.float32)

def reference(diag_block, panel, trailing):
    lower = jnp.linalg.cholesky(diag_block)
    ident = jnp.eye(BLOCK, dtype=jnp.float32)
    inverse = lax.linalg.triangular_solve(lower, ident, left_side=True, lower=True)
    factor_panel = jnp.dot(panel.astype(jnp.float32), inverse.T.astype(jnp.float32), precision=lax.Precision.HIGHEST, preferred_element_type=jnp.float32)
    step = min(TRAIL, 1024)
    count = TRAIL // step
    trail_blocks = trailing.reshape(count, step, TRAIL)
    panel_blocks = factor_panel.reshape(count, step, BLOCK)

    def update(pair):
        return pair[0] - outer_rows(pair[1], factor_panel)
    schur = lax.map(update, (trail_blocks, panel_blocks)).reshape(TRAIL, TRAIL)
    return (lower, factor_panel, schur)
```

```python
import jax
import jax.numpy as jnp
from jax import lax
from jax.experimental import pallas as pl
from jax.experimental.pallas import tpu as pltpu
from jax.sharding import PartitionSpec as P

ORDER = 512
BAND = 32


def split3(x):
    high = x.astype(jnp.bfloat16)
    rest = x - high.astype(jnp.float32)
    mid = rest.astype(jnp.bfloat16)
    low = (rest - mid.astype(jnp.float32)).astype(jnp.bfloat16)
    return high, mid, low


def spread(rows, which):
    return jnp.broadcast_to(rows[which : which + 1, :], (8, 128))


def band_step(inv_ref, upper_ref, base, part):
    start = pl.multiple_of(base + BAND * part, BAND)
    group = pl.multiple_of(base, 128)
    tiles = BAND // 8
    here = inv_ref[pl.ds(start, BAND), pl.ds(group, 128)]
    lane = lax.broadcasted_iota(jnp.int32, (8, 128), 1)
    sub = lax.broadcasted_iota(jnp.int32, (8, 128), 0)
    cols = []
    for j in range(BAND):
        first = j // 8
        wide = jnp.broadcast_to(
            here[8 * first :, BAND * part + j : BAND * part + j + 1], (BAND - 8 * first, 128)
        )
        cols.append([None] * first + [wide[8 * t : 8 * t + 8] for t in range(tiles - first)])
    rows = []
    for q in range(4):
        strip = inv_ref[pl.ds(start, BAND), 128 * q : 128 * q + 128]
        rows.append([strip[8 * t : 8 * t + 8] for t in range(tiles)])
    rows.append(
        [jnp.where(lane == sub + (BAND * part + 8 * t), 1.0, 0.0) for t in range(tiles)]
    )
    for j in range(BAND):
        tj, sj = j // 8, j % 8
        scale = lax.rsqrt(spread(cols[j][tj], sj))
        factor = [None if col is None else col * scale for col in cols[j]]
        for k in range(j + 1, BAND):
            weight = spread(factor[k // 8], k % 8)
            for t in range(k // 8, tiles):
                cols[k][t] = cols[k][t] - factor[t] * weight
        below = jnp.where(sub > sj, factor[tj], 0.0)
        for strip in rows:
            row = spread(strip[tj], sj) * scale
            strip[tj] = jnp.where(sub == sj, row, strip[tj] - below * row)
            for t in range(tj + 1, tiles):
                strip[t] = strip[t] - factor[t] * row
    lanes = lax.broadcasted_iota(jnp.int32, (BAND, 128), 1)
    subs = lax.broadcasted_iota(jnp.int32, (BAND, 128), 0)
    solved = [jnp.concatenate(strip, axis=0) for strip in rows]
    right, whole = [], []
    for q in range(4):
        col = lanes + 128 * q
        upper_ref[pl.ds(start, BAND), 128 * q : 128 * q + 128] = jnp.where(
            col >= subs + start, solved[q], 0.0
        )
        right.append(jnp.where(col >= start + BAND, solved[q], 0.0))
        whole.append(jnp.where((col >= start) & (col < start + BAND), solved[4], solved[q]))
    right, whole = jnp.concatenate(right, axis=1), jnp.concatenate(whole, axis=1)
    uh, um, ul = split3(right)
    wh, wm, wl = split3(whole)
    product = lax.dot_general(
        jnp.concatenate([uh, uh, uh, um, um, ul, um, ul], axis=0),
        jnp.concatenate([wh, wm, wl, wh, wm, wh, wl, wm], axis=0),
        (((0,), (0,)), ((), ())),
        preferred_element_type=jnp.float32,
    )
    col = lax.broadcasted_iota(jnp.int32, (ORDER, ORDER), 1)
    inv_ref[...] = jnp.where((col >= start) & (col < start + BAND), 0.0, inv_ref[...]) - product
    inv_ref[pl.ds(start, BAND), :] = whole


def factor_kernel(diag_ref, inv_ref, upper_ref):
    inv_ref[...] = diag_ref[...]

    @pl.loop(0, ORDER // 128)
    def _(block):
        for part in range(128 // BAND):
            band_step(inv_ref, upper_ref, block * 128, part)


def factor_and_invert(diag):
    return pl.pallas_call(
        factor_kernel,
        out_shape=(jax.ShapeDtypeStruct((ORDER, ORDER), jnp.float32),) * 2,
        in_specs=[pl.BlockSpec(memory_space=pltpu.VMEM)],
        out_specs=(pl.BlockSpec(memory_space=pltpu.VMEM),) * 2,
        name="factor_and_invert",
    )(diag)


def laid_out(pieces, dim):
    dims = list(pieces.shape[1:])
    dims[dim] *= pieces.shape[0]
    return jnp.moveaxis(pieces, 0, dim).reshape(dims)


def copy_for_each(array, axis):
    count = lax.axis_size(axis)
    return lax.all_to_all(
        jnp.broadcast_to(array[None], (count, *array.shape)), axis, 0, 0, tiled=True
    )


def collect(array, axis, dim):
    return laid_out(copy_for_each(array, axis), dim)


def padded_to(lines, count):
    spare = -lines.shape[0] % count
    if not spare:
        return lines
    return jnp.concatenate([lines, jnp.zeros((spare, *lines.shape[1:]), lines.dtype)])


def broadcast_by_parts(array, axis, root):
    lines = jnp.where(lax.axis_index(axis) == root, array, jnp.zeros_like(array)).reshape(
        -1, *array.shape[1:][-1:]
    )
    padded = padded_to(lines, lax.axis_size(axis))
    own = lax.psum_scatter(padded, axis, scatter_dimension=0, tiled=True)
    return lax.all_gather(own, axis, axis=0, tiled=True)[: len(lines)].reshape(array.shape)


def outer_rows(left, right):
    return lax.dot_general(
        left,
        right,
        (((1,), (1,)), ((), ())),
        precision=lax.Precision.HIGHEST,
        preferred_element_type=jnp.float32,
    )


def exact_dot(left, right):
    return jnp.dot(left, right, precision=lax.Precision.HIGHEST, preferred_element_type=jnp.float32)


def local(diag_block, panel, trailing):
    n_depth = lax.axis_size("depth")
    whole_diag = collect(diag_block, ("row", "col"), 0)
    inverse, upper = factor_and_invert(whole_diag)
    inv_trans = inverse.T
    own_rows = diag_block.shape[0]
    factor_diag = lax.dynamic_slice_in_dim(
        upper, lax.axis_index(("row", "col")) * own_rows, own_rows, 1
    ).T
    layer = lax.axis_index("depth")
    col_index = lax.axis_index("col")
    width = panel.shape[1]
    full_panel = lax.all_gather(panel, "depth", axis=1, tiled=True)
    solved = exact_dot(full_panel, inv_trans)
    factor_panel = lax.dynamic_slice_in_dim(solved, layer * width, width, 1)
    row_full = lax.all_gather(solved, "col", axis=0, tiled=True)
    rows_out = trailing.shape[0]
    span = row_full.shape[0]
    block_index = col_index * n_depth + layer
    root = block_index * rows_out // span
    col_rows = broadcast_by_parts(row_full, "row", root)
    update = outer_rows(col_rows, row_full)
    schur = trailing - update
    return (factor_diag, factor_panel, schur)


def solution(mesh):
    in_specs = (P(("row", "col"), None), P(("row", "col"), "depth"), P(("col", "depth"), "row"))
    out_specs = (P(("row", "col"), None), P(("row", "col"), "depth"), P(("col", "depth"), "row"))
    return jax.shard_map(local, mesh=mesh, in_specs=in_specs, out_specs=out_specs, check_vma=False)
```

```python
import functools

import jax
import jax.numpy as jnp
from jax import lax
from jax.experimental import pallas as pl
from jax.experimental.pallas import tpu as pltpu
from jax.sharding import PartitionSpec as P

ORDER = 512
BAND = 32


def split3(x):
    high = x.astype(jnp.bfloat16)
    rest = x - high.astype(jnp.float32)
    mid = rest.astype(jnp.bfloat16)
    low = (rest - mid.astype(jnp.float32)).astype(jnp.bfloat16)
    return high, mid, low


def spread(rows, which):
    return jnp.broadcast_to(rows[which : which + 1, :], (8, 128))


def band_step(inv_ref, upper_ref, base, part):
    start = pl.multiple_of(base + BAND * part, BAND)
    group = pl.multiple_of(base, 128)
    tiles = BAND // 8
    here = inv_ref[pl.ds(start, BAND), pl.ds(group, 128)]
    lane = lax.broadcasted_iota(jnp.int32, (8, 128), 1)
    sub = lax.broadcasted_iota(jnp.int32, (8, 128), 0)
    cols = []
    for j in range(BAND):
        first = j // 8
        wide = jnp.broadcast_to(
            here[8 * first :, BAND * part + j : BAND * part + j + 1], (BAND - 8 * first, 128)
        )
        cols.append([None] * first + [wide[8 * t : 8 * t + 8] for t in range(tiles - first)])
    rows = []
    for q in range(4):
        strip = inv_ref[pl.ds(start, BAND), 128 * q : 128 * q + 128]
        rows.append([strip[8 * t : 8 * t + 8] for t in range(tiles)])
    rows.append(
        [jnp.where(lane == sub + (BAND * part + 8 * t), 1.0, 0.0) for t in range(tiles)]
    )
    for j in range(BAND):
        tj, sj = j // 8, j % 8
        scale = lax.rsqrt(spread(cols[j][tj], sj))
        factor = [None if col is None else col * scale for col in cols[j]]
        for k in range(j + 1, BAND):
            weight = spread(factor[k // 8], k % 8)
            for t in range(k // 8, tiles):
                cols[k][t] = cols[k][t] - factor[t] * weight
        below = jnp.where(sub > sj, factor[tj], 0.0)
        for strip in rows:
            row = spread(strip[tj], sj) * scale
            strip[tj] = jnp.where(sub == sj, row, strip[tj] - below * row)
            for t in range(tj + 1, tiles):
                strip[t] = strip[t] - factor[t] * row
    lanes = lax.broadcasted_iota(jnp.int32, (BAND, 128), 1)
    subs = lax.broadcasted_iota(jnp.int32, (BAND, 128), 0)
    solved = [jnp.concatenate(strip, axis=0) for strip in rows]
    right, whole = [], []
    for q in range(4):
        col = lanes + 128 * q
        upper_ref[pl.ds(start, BAND), 128 * q : 128 * q + 128] = jnp.where(
            col >= subs + start, solved[q], 0.0
        )
        right.append(jnp.where(col >= start + BAND, solved[q], 0.0))
        whole.append(jnp.where((col >= start) & (col < start + BAND), solved[4], solved[q]))
    right, whole = jnp.concatenate(right, axis=1), jnp.concatenate(whole, axis=1)
    uh, um, ul = split3(right)
    wh, wm, wl = split3(whole)
    product = lax.dot_general(
        jnp.concatenate([uh, uh, uh, um, um, ul, um, ul], axis=0),
        jnp.concatenate([wh, wm, wl, wh, wm, wh, wl, wm], axis=0),
        (((0,), (0,)), ((), ())),
        preferred_element_type=jnp.float32,
    )
    col = lax.broadcasted_iota(jnp.int32, (ORDER, ORDER), 1)
    inv_ref[...] = jnp.where((col >= start) & (col < start + BAND), 0.0, inv_ref[...]) - product
    inv_ref[pl.ds(start, BAND), :] = whole


MESH = pl.DeviceIdType.MESH
F32 = jnp.float32
BF16 = jnp.bfloat16
SHIFTS = sorted(
    [(i, j) for i in range(4) for j in range(4) if i or j],
    key=lambda s: -(min(s[0], 4 - s[0]) + min(s[1], 4 - s[1])),
)


def exchange_kernel(
    diag_ref,
    panel_ref,
    cols_ref,
    rows_ref,
    inv_out,
    slab_ref,
    gathered,
    piece,
    turned,
    inv_ref,
    upper_ref,
    local_sem,
    keep_sem,
    z_send,
    z_recv,
    xy_send,
    xy_recv,
    pair_send,
    pair_recv,
    turn_send,
    turn_recv,
    rz_send,
    rz_recv,
    rp_send,
    rp_recv,
    c_send,
    c_recv,
    out_sem,
):
    row, c, d = lax.axis_index("row"), lax.axis_index("col"), lax.axis_index("depth")
    z, k = row // 2, row % 2
    block = 4 * c + d
    turn_c, turn_d = row // 4, row % 4
    fixed = block == row

    def at(row_id, col_id, depth_id):
        return {"row": row_id, "col": col_id, "depth": depth_id}

    def remote(src, dst, send, recv, where):
        return pltpu.make_async_remote_copy(
            src_ref=src, dst_ref=dst, send_sem=send, recv_sem=recv,
            device_id=where, device_id_type=MESH,
        )

    lane = pl.multiple_of(d * 128, 128)
    load_diag = pltpu.make_async_copy(
        diag_ref.at[:, pl.ds(lane, 128)], gathered.at[k, c, d, z], local_sem.at[0]
    )
    load_diag.start()
    load_piece = pltpu.make_async_copy(panel_ref, piece, local_sem.at[1])
    load_piece.start()

    @pl.when(fixed)
    def _():
        pltpu.make_async_copy(panel_ref, turned, local_sem.at[2]).start()

    barrier = pltpu.get_barrier_semaphore()

    def greet(where):
        pl.semaphore_signal(barrier, inc=1, device_id=where, device_id_type=MESH)

    z_peers = [at(2 * ((z + s) % 8) + k, c, d) for s in range(8)]
    xy_peers = [at(row, (c + i) % 4, (d + j) % 4) for i, j in SHIFTS]
    partner = at(2 * z + 1 - k, c, d)
    turn_peer = at(block, turn_c, turn_d)
    for s in range(1, 8):
        greet(z_peers[s])
    for peer in xy_peers:
        greet(peer)
    greet(partner)

    @pl.when(jnp.logical_not(fixed))
    def _():
        greet(turn_peer)

    @pl.when(fixed)
    def _():
        pl.semaphore_wait(barrier, 23)

    @pl.when(jnp.logical_not(fixed))
    def _():
        pl.semaphore_wait(barrier, 24)

    load_diag.wait()
    z_copies = [
        remote(gathered.at[k, c, d, z], gathered.at[k, c, d, z], z_send.at[s], z_recv.at[s], z_peers[s])
        for s in range(1, 8)
    ]
    for copy in z_copies:
        copy.start()
    load_piece.wait()

    @pl.when(jnp.logical_not(fixed))
    def _():
        remote(piece, turned, turn_send, turn_recv, turn_peer).start()

    keep_piece = pltpu.make_async_copy(piece, cols_ref.at[c, d], keep_sem.at[0])
    keep_piece.start()
    for s in range(1, 8):
        from_z = (z - s + 8) % 8
        remote(
            gathered.at[k, c, d, from_z], gathered.at[k, c, d, from_z],
            z_send.at[s], z_recv.at[s], z_peers[s],
        ).wait_recv()

    xy_copies = [
        remote(gathered.at[k, c, d], gathered.at[k, c, d], xy_send.at[n], xy_recv.at[n], xy_peers[n])
        for n in range(15)
    ]
    for copy in xy_copies:
        copy.start()
    pair_copies = [
        remote(gathered.at[k, c, d], gathered.at[k, c, d], pair_send.at[15], pair_recv.at[15], partner)
    ]
    pair_copies[0].start()

    @pl.when(fixed)
    def _():
        pltpu.make_async_copy(panel_ref, turned, local_sem.at[2]).wait()

    @pl.when(jnp.logical_not(fixed))
    def _():
        remote(piece, turned, turn_send, turn_recv, turn_peer).wait_recv()

    rz_copies = [
        remote(turned, rows_ref.at[row], rz_send.at[s], rz_recv.at[s], z_peers[s])
        for s in (4, 3, 5, 2, 6, 1, 7)
    ]
    for copy in rz_copies:
        copy.start()
    keep_turned = pltpu.make_async_copy(turned, rows_ref.at[row], keep_sem.at[1])
    keep_turned.start()
    rp_copies = [remote(turned, rows_ref.at[row], rp_send.at[0], rp_recv.at[0], partner)]
    rp_copies[0].start()

    for n in reversed(range(15)):
        i, j = SHIFTS[n]
        fc, fd = (c - i + 4) % 4, (d - j + 4) % 4
        remote(
            gathered.at[k, fc, fd], gathered.at[k, fc, fd], xy_send.at[n], xy_recv.at[n], xy_peers[n]
        ).wait_recv()
        copy = remote(
            gathered.at[k, fc, fd], gathered.at[k, fc, fd], pair_send.at[n], pair_recv.at[n], partner
        )
        copy.start()
        pair_copies.append(copy)

    c_copies = [
        remote(piece, cols_ref.at[c, d], c_send.at[n], c_recv.at[n], xy_peers[n]) for n in range(15)
    ]
    for copy in c_copies:
        copy.start()
    for n in range(16):
        i, j = (0, 0) if n == 15 else SHIFTS[n]
        fc, fd = (c - i + 4) % 4, (d - j + 4) % 4
        remote(
            gathered.at[1 - k, fc, fd], gathered.at[1 - k, fc, fd],
            pair_send.at[n], pair_recv.at[n], partner,
        ).wait_recv()

    for fk in range(2):
        for fc in range(4):
            for fd in range(4):
                for fz in range(8):
                    first = (2 * fz + fk) * 32 + fc * 8
                    inv_ref[first : first + 8, 128 * fd : 128 * fd + 128] = gathered[fk, fc, fd, fz]

    def forward(s):
        from_row = 2 * ((z - s + 8) % 8) + k
        return (
            remote(turned, rows_ref.at[from_row], rz_send.at[s], rz_recv.at[s], z_peers[s]),
            remote(rows_ref.at[from_row], rows_ref.at[from_row], rp_send.at[s], rp_recv.at[s], partner),
        )

    @pl.loop(0, ORDER // 128)
    def _(step):
        for part in range(128 // BAND):
            band_step(inv_ref, upper_ref, step * 128, part)

    store_inv = pltpu.make_async_copy(inv_ref, inv_out, out_sem)
    store_inv.start()
    for s in range(1, 8):
        arrived, onward = forward(s)
        arrived.wait_recv()
        onward.start()

    mine = row * 4 + c
    group = pl.multiple_of((mine // 16) * 128, 128)
    upper_ref[:128, :] = upper_ref[:, pl.ds(group, 128)].T
    slab_ref[...] = upper_ref[pl.ds(pl.multiple_of((mine % 16) * 8, 8), 8), :]

    for n in range(15):
        i, j = SHIFTS[n]
        fc, fd = (c - i + 4) % 4, (d - j + 4) % 4
        remote(piece, cols_ref.at[fc, fd], c_send.at[n], c_recv.at[n], xy_peers[n]).wait_recv()
    for s in range(8):
        from_row = 2 * ((z - s + 8) % 8) + 1 - k
        remote(
            rows_ref.at[from_row], rows_ref.at[from_row], rp_send.at[s], rp_recv.at[s], partner
        ).wait_recv()
    for s in range(1, 8):
        forward(s)[1].wait_send()

    @pl.when(jnp.logical_not(fixed))
    def _():
        remote(piece, turned, turn_send, turn_recv, turn_peer).wait_send()

    for copy in z_copies + xy_copies + pair_copies + rz_copies + rp_copies + c_copies:
        copy.wait_send()
    keep_piece.wait()
    keep_turned.wait()
    store_inv.wait()


def exchange_and_factor(diag_block, panel):
    hbm = pl.BlockSpec(memory_space=pltpu.MemorySpace.HBM)
    dma = pltpu.SemaphoreType.DMA
    return pl.pallas_call(
        exchange_kernel,
        out_shape=(
            jax.ShapeDtypeStruct((4, 4, 256, 128), F32),
            jax.ShapeDtypeStruct((16, 256, 128), F32),
            jax.ShapeDtypeStruct((ORDER, ORDER), F32),
            jax.ShapeDtypeStruct((8, ORDER), F32),
        ),
        in_specs=[hbm, hbm],
        out_specs=(hbm, hbm, hbm, pl.BlockSpec(memory_space=pltpu.VMEM)),
        scratch_shapes=[
            pltpu.VMEM((2, 4, 4, 8, 8, 128), F32),
            pltpu.VMEM((256, 128), F32),
            pltpu.VMEM((256, 128), F32),
            pltpu.VMEM((ORDER, ORDER), F32),
            pltpu.VMEM((ORDER, ORDER), F32),
            dma((3,)),
            dma((2,)),
            dma((8,)),
            dma((8,)),
            dma((15,)),
            dma((15,)),
            dma((16,)),
            dma((16,)),
            dma,
            dma,
            dma((8,)),
            dma((8,)),
            dma((8,)),
            dma((8,)),
            dma((15,)),
            dma((15,)),
            dma,
        ],
        compiler_params=pltpu.CompilerParams(collective_id=0, has_side_effects=True),
        name="exchange_and_factor",
    )(diag_block, panel)


def split2(x):
    high = x.astype(BF16)
    return high, (x - high.astype(F32)).astype(BF16)


def dot_nt(left, right):
    lh, ll = left
    rh, rl = right
    dims = (((1,), (1,)), ((), ()))
    dot = functools.partial(lax.dot_general, dimension_numbers=dims, preferred_element_type=F32)
    return dot(lh, rh) + dot(lh, rl) + dot(ll, rh)


TILE = 256


def update_kernel(
    place_ref, cols_ref, rows_ref, inv_ref, slab_ref, trail_ref,
    slab_out, panel_out, schur_ref, ih_ref, il_ref, sh_ref, sl_ref,
):
    step = pl.program_id(0)

    def solve(pieces):
        whole = jnp.concatenate(pieces, axis=1)
        ph, pl_ = split2(whole)
        left = dot_nt((ph[:, :256], pl_[:, :256]), (ih_ref[:256, :256], il_ref[:256, :256]))
        right = dot_nt((ph, pl_), (ih_ref[256:, :], il_ref[256:, :]))
        return jnp.concatenate([left, right], axis=1)

    @pl.when(step == 0)
    def _():
        slab_out[...] = slab_ref[...]
        ih_ref[...], il_ref[...] = split2(inv_ref[...])
        for q in range(4):
            part = solve([cols_ref[q, e] for e in range(4)])
            sh, sl = split2(part)
            sh_ref[256 * q : 256 * q + 256, :] = sh
            sl_ref[256 * q : 256 * q + 256, :] = sl

            @pl.when(place_ref[0] == q)
            def _():
                for e in range(4):

                    @pl.when(place_ref[1] == e)
                    def _():
                        panel_out[...] = part[:, 128 * e : 128 * e + 128]

    mine = split2(solve([rows_ref[4 * step + e] for e in range(4)]))
    schur_ref[...] = trail_ref[...] - dot_nt(mine, (sh_ref[...], sl_ref[...]))


def solve_and_update(cols, rows, inverse, slab, trailing):
    place = jnp.stack([lax.axis_index("col"), lax.axis_index("depth")]).astype(jnp.int32)
    whole = lambda *shape: pl.BlockSpec(
        shape, lambda i, p: (0,) * len(shape), pipeline_mode=pl.Buffered(1)
    )
    tile = pl.BlockSpec((TILE, 1024), lambda i, p: (i, 0))
    return pl.pallas_call(
        update_kernel,
        grid_spec=pltpu.PrefetchScalarGridSpec(
            num_scalar_prefetch=1,
            grid=(1024 // TILE,),
            in_specs=[whole(4, 4, 256, 128), whole(16, 256, 128), whole(ORDER, ORDER), whole(8, ORDER), tile],
            out_specs=(
                pl.BlockSpec((8, ORDER), lambda i, p: (0, 0)),
                pl.BlockSpec((256, 128), lambda i, p: (0, 0)),
                tile,
            ),
            scratch_shapes=[
                pltpu.VMEM((ORDER, ORDER), BF16),
                pltpu.VMEM((ORDER, ORDER), BF16),
                pltpu.VMEM((1024, ORDER), BF16),
                pltpu.VMEM((1024, ORDER), BF16),
            ],
        ),
        out_shape=(
            jax.ShapeDtypeStruct((8, ORDER), F32),
            jax.ShapeDtypeStruct((256, 128), F32),
            jax.ShapeDtypeStruct((1024, 1024), F32),
        ),
        name="solve_and_update",
    )(place, cols, rows, inverse, slab, trailing)


def local(diag_block, panel, trailing):
    cols, rows, inverse, slab = exchange_and_factor(diag_block, panel)
    return solve_and_update(cols, rows, inverse, slab, trailing)


def solution(mesh):
    in_specs = (P(("row", "col"), None), P(("row", "col"), "depth"), P(("col", "depth"), "row"))
    out_specs = (P(("row", "col"), None), P(("row", "col"), "depth"), P(("col", "depth"), "row"))
    return jax.shard_map(local, mesh=mesh, in_specs=in_specs, out_specs=out_specs, check_vma=False)
```

```python
import functools

import jax
import jax.numpy as jnp
from jax import lax
from jax.experimental import pallas as pl
from jax.experimental.pallas import tpu as pltpu
from jax.sharding import PartitionSpec as P

ORDER = 512
BAND = 32


def split3(x):
    high = x.astype(jnp.bfloat16)
    rest = x - high.astype(jnp.float32)
    mid = rest.astype(jnp.bfloat16)
    low = (rest - mid.astype(jnp.float32)).astype(jnp.bfloat16)
    return high, mid, low


def spread(rows, which):
    return jnp.broadcast_to(rows[which : which + 1, :], (8, 128))


def band_step(inv_ref, upper_ref, base, part):
    start = pl.multiple_of(base + BAND * part, BAND)
    group = pl.multiple_of(base, 128)
    tiles = BAND // 8
    here = inv_ref[pl.ds(start, BAND), pl.ds(group, 128)]
    lane = lax.broadcasted_iota(jnp.int32, (8, 128), 1)
    sub = lax.broadcasted_iota(jnp.int32, (8, 128), 0)
    cols = []
    for j in range(BAND):
        first = j // 8
        wide = jnp.broadcast_to(
            here[8 * first :, BAND * part + j : BAND * part + j + 1], (BAND - 8 * first, 128)
        )
        cols.append([None] * first + [wide[8 * t : 8 * t + 8] for t in range(tiles - first)])
    rows = []
    for q in range(4):
        strip = inv_ref[pl.ds(start, BAND), 128 * q : 128 * q + 128]
        rows.append([strip[8 * t : 8 * t + 8] for t in range(tiles)])
    rows.append(
        [jnp.where(lane == sub + (BAND * part + 8 * t), 1.0, 0.0) for t in range(tiles)]
    )
    for j in range(BAND):
        tj, sj = j // 8, j % 8
        scale = lax.rsqrt(spread(cols[j][tj], sj))
        factor = [None if col is None else col * scale for col in cols[j]]
        for k in range(j + 1, BAND):
            weight = spread(factor[k // 8], k % 8)
            for t in range(k // 8, tiles):
                cols[k][t] = cols[k][t] - factor[t] * weight
        below = jnp.where(sub > sj, factor[tj], 0.0)
        for strip in rows:
            row = spread(strip[tj], sj) * scale
            strip[tj] = jnp.where(sub == sj, row, strip[tj] - below * row)
            for t in range(tj + 1, tiles):
                strip[t] = strip[t] - factor[t] * row
    lanes = lax.broadcasted_iota(jnp.int32, (BAND, 128), 1)
    subs = lax.broadcasted_iota(jnp.int32, (BAND, 128), 0)
    solved = [jnp.concatenate(strip, axis=0) for strip in rows]
    right, whole = [], []
    for q in range(4):
        col = lanes + 128 * q
        upper_ref[pl.ds(start, BAND), 128 * q : 128 * q + 128] = jnp.where(
            col >= subs + start, solved[q], 0.0
        )
        right.append(jnp.where(col >= start + BAND, solved[q], 0.0))
        whole.append(jnp.where((col >= start) & (col < start + BAND), solved[4], solved[q]))
    right, whole = jnp.concatenate(right, axis=1), jnp.concatenate(whole, axis=1)
    uh, um, ul = split3(right)
    wh, wm, wl = split3(whole)
    product = lax.dot_general(
        jnp.concatenate([uh, uh, uh, um, um, ul, um, ul], axis=0),
        jnp.concatenate([wh, wm, wl, wh, wm, wh, wl, wm], axis=0),
        (((0,), (0,)), ((), ())),
        preferred_element_type=jnp.float32,
    )
    col = lax.broadcasted_iota(jnp.int32, (ORDER, ORDER), 1)
    inv_ref[...] = jnp.where((col >= start) & (col < start + BAND), 0.0, inv_ref[...]) - product
    inv_ref[pl.ds(start, BAND), :] = whole


MESH = pl.DeviceIdType.MESH
F32 = jnp.float32
BF16 = jnp.bfloat16
SHIFTS = sorted(
    [(i, j) for i in range(4) for j in range(4) if i or j],
    key=lambda s: -(min(s[0], 4 - s[0]) + min(s[1], 4 - s[1])),
)

FAR_FIRST = (4, 3, 5, 2, 6, 1, 7)


def exchange_kernel(
    diag_ref,
    panel_ref,
    cols_ref,
    rows_ref,
    inv_out,
    slab_ref,
    gathered,
    piece,
    turned,
    inv_ref,
    upper_ref,
    local_sem,
    keep_sem,
    z_send,
    z_recv,
    xy_send,
    xy_recv,
    pair_send,
    pair_recv,
    turn_send,
    turn_recv,
    rz_send,
    rz_recv,
    rp_send,
    rp_recv,
    c_send,
    c_recv,
    out_sem,
):
    row, c, d = lax.axis_index("row"), lax.axis_index("col"), lax.axis_index("depth")
    z, k = row // 2, row % 2
    block = 4 * c + d
    turn_c, turn_d = row // 4, row % 4
    fixed = block == row

    def at(row_id, col_id, depth_id):
        return {"row": row_id, "col": col_id, "depth": depth_id}

    def remote(src, dst, send, recv, where):
        return pltpu.make_async_remote_copy(
            src_ref=src, dst_ref=dst, send_sem=send, recv_sem=recv,
            device_id=where, device_id_type=MESH,
        )

    lane = pl.multiple_of(d * 128, 128)
    load_diag = pltpu.make_async_copy(
        diag_ref.at[:, pl.ds(lane, 128)], gathered.at[k, c, d, z], local_sem.at[0]
    )
    load_diag.start()
    load_piece = pltpu.make_async_copy(panel_ref, piece, local_sem.at[1])
    load_piece.start()

    @pl.when(fixed)
    def _():
        pltpu.make_async_copy(panel_ref, turned, local_sem.at[2]).start()

    barrier = pltpu.get_barrier_semaphore()

    def greet(where):
        pl.semaphore_signal(barrier, inc=1, device_id=where, device_id_type=MESH)

    z_peers = [at(2 * ((z + s) % 8) + k, c, d) for s in range(8)]
    xy_peers = [at(row, (c + i) % 4, (d + j) % 4) for i, j in SHIFTS]
    x_peers = [at(row, (c + i) % 4, d) for i in range(4)]
    y_peers = [at(row, c, (d + j) % 4) for j in range(4)]
    partner = at(2 * z + 1 - k, c, d)
    turn_peer = at(block, turn_c, turn_d)
    for s in FAR_FIRST:
        greet(z_peers[s])
    for peer in xy_peers:
        greet(peer)
    greet(partner)

    @pl.when(jnp.logical_not(fixed))
    def _():
        greet(turn_peer)

    @pl.when(fixed)
    def _():
        pl.semaphore_wait(barrier, 23)

    @pl.when(jnp.logical_not(fixed))
    def _():
        pl.semaphore_wait(barrier, 24)

    load_diag.wait()
    sent = []

    def start(copy):
        copy.start()
        sent.append(copy)

    for s in FAR_FIRST:
        start(remote(
            gathered.at[k, c, d, z], gathered.at[k, c, d, z], z_send.at[s], z_recv.at[s], z_peers[s]
        ))

    load_piece.wait()

    @pl.when(jnp.logical_not(fixed))
    def _():
        remote(piece, turned, turn_send, turn_recv, turn_peer).start()

    halves = [piece.at[:128], piece.at[128:]]
    own_slots = [cols_ref.at[0, d, c], cols_ref.at[1, c, d]]
    keeps = [pltpu.make_async_copy(halves[h], own_slots[h], keep_sem.at[h]) for h in range(2)]
    for h in range(2):
        for s in (2, 1, 3):
            peer = (x_peers, y_peers)[h][s]
            start(remote(halves[h], own_slots[h], c_send.at[h, s], c_recv.at[h, s], peer))
        keeps[h].start()

    for s in range(1, 8):
        from_z = (z - s + 8) % 8
        remote(
            gathered.at[k, c, d, from_z], gathered.at[k, c, d, from_z],
            z_send.at[s], z_recv.at[s], z_peers[s],
        ).wait_recv()

    for n in range(15):
        start(remote(
            gathered.at[k, c, d], gathered.at[k, c, d], xy_send.at[n], xy_recv.at[n], xy_peers[n]
        ))
    start(remote(
        gathered.at[k, c, d], gathered.at[k, c, d], pair_send.at[15], pair_recv.at[15], partner
    ))

    @pl.when(fixed)
    def _():
        pltpu.make_async_copy(panel_ref, turned, local_sem.at[2]).wait()

    @pl.when(jnp.logical_not(fixed))
    def _():
        remote(piece, turned, turn_send, turn_recv, turn_peer).wait_recv()

    for s in (2, 6, 1, 7):
        start(remote(turned, rows_ref.at[row], rz_send.at[s], rz_recv.at[s], z_peers[s]))
    keep_turned = pltpu.make_async_copy(turned, rows_ref.at[row], keep_sem.at[2])
    keep_turned.start()
    start(remote(turned, rows_ref.at[row], rp_send.at[0], rp_recv.at[0], partner))

    for n in reversed(range(15)):
        i, j = SHIFTS[n]
        fc, fd = (c - i + 4) % 4, (d - j + 4) % 4
        remote(
            gathered.at[k, fc, fd], gathered.at[k, fc, fd], xy_send.at[n], xy_recv.at[n], xy_peers[n]
        ).wait_recv()
        start(remote(
            gathered.at[k, fc, fd], gathered.at[k, fc, fd], pair_send.at[n], pair_recv.at[n], partner
        ))
    for n in reversed(range(16)):
        i, j = (0, 0) if n == 15 else SHIFTS[n]
        fc, fd = (c - i + 4) % 4, (d - j + 4) % 4
        remote(
            gathered.at[1 - k, fc, fd], gathered.at[1 - k, fc, fd],
            pair_send.at[n], pair_recv.at[n], partner,
        ).wait_recv()

    def half_from(h, s):
        if h == 0:
            return cols_ref.at[0, d, (c - s + 4) % 4]
        return cols_ref.at[1, c, (d - s + 4) % 4]

    for h in range(2):
        keeps[h].wait()
        for s in range(1, 4):
            slot = half_from(h, s)
            remote(slot, slot, c_send.at[h, s], c_recv.at[h, s], partner).wait_recv()
        line = cols_ref.at[h, (d, c)[h]]
        for s in (2, 1, 3):
            peer = (y_peers, x_peers)[h][s]
            start(remote(line, line, c_send.at[h, 3 + s], c_recv.at[h, 3 + s], peer))

    def from_row(s):
        return 2 * ((z - s + 8) % 8) + k

    def arrive(s):
        slot = rows_ref.at[from_row(s)]
        remote(slot, slot, rz_send.at[s], rz_recv.at[s], partner).wait_recv()

    def pass_on(s):
        slot = rows_ref.at[from_row(s)]
        start(remote(slot, slot, rp_send.at[s], rp_recv.at[s], partner))

    for s, side in ((2, 0), (6, 1)):
        arrive(s)
        slot = rows_ref.at[from_row(s)]
        part = rows_ref.at[from_row(s), pl.ds(128 * side, 128)]
        ahead, twice = ((1, 2), (7, 6))[side]
        start(remote(part, part, rz_send.at[4 + 4 * side], rz_recv.at[4 + 4 * side], z_peers[twice]))
        start(remote(slot, slot, rz_send.at[3 + 2 * side], rz_recv.at[3 + 2 * side], z_peers[ahead]))
        pass_on(s)
    for s in (1, 7):
        arrive(s)
        pass_on(s)

    for fk in range(2):
        for fc in range(4):
            for fd in range(4):
                for fz in range(8):
                    first = (2 * fz + fk) * 32 + fc * 8
                    inv_ref[first : first + 8, 128 * fd : 128 * fd + 128] = gathered[fk, fc, fd, fz]

    @pl.loop(0, ORDER // 128)
    def _(step):
        for part in range(128 // BAND):
            band_step(inv_ref, upper_ref, step * 128, part)

    store_inv = pltpu.make_async_copy(inv_ref, inv_out, out_sem)
    store_inv.start()
    for s in (3, 5):
        arrive(s)
        pass_on(s)
    for side in range(2):
        part = rows_ref.at[from_row(4), pl.ds(128 * side, 128)]
        sem = 4 + 4 * side
        remote(part, part, rz_send.at[sem], rz_recv.at[sem], partner).wait_recv()
    pass_on(4)

    mine = row * 4 + c
    group = pl.multiple_of((mine // 16) * 128, 128)
    upper_ref[:128, :] = upper_ref[:, pl.ds(group, 128)].T
    slab_ref[...] = upper_ref[pl.ds(pl.multiple_of((mine % 16) * 8, 8), 8), :]

    for h in range(2):
        for s in range(1, 4):
            line = cols_ref.at[h, ((d, c)[h] - s + 4) % 4]
            remote(line, line, c_send.at[h, 3 + s], c_recv.at[h, 3 + s], partner).wait_recv()
    for s in range(8):
        slot = rows_ref.at[2 * ((z - s + 8) % 8) + 1 - k]
        remote(slot, slot, rp_send.at[s], rp_recv.at[s], partner).wait_recv()

    @pl.when(jnp.logical_not(fixed))
    def _():
        remote(piece, turned, turn_send, turn_recv, turn_peer).wait_send()

    for copy in sent:
        copy.wait_send()
    keep_turned.wait()
    store_inv.wait()


def exchange_and_factor(diag_block, panel):
    hbm = pl.BlockSpec(memory_space=pltpu.MemorySpace.HBM)
    dma = pltpu.SemaphoreType.DMA
    return pl.pallas_call(
        exchange_kernel,
        out_shape=(
            jax.ShapeDtypeStruct((2, 4, 4, 128, 128), F32),
            jax.ShapeDtypeStruct((16, 256, 128), F32),
            jax.ShapeDtypeStruct((ORDER, ORDER), F32),
            jax.ShapeDtypeStruct((8, ORDER), F32),
        ),
        in_specs=[hbm, hbm],
        out_specs=(hbm, hbm, hbm, pl.BlockSpec(memory_space=pltpu.VMEM)),
        scratch_shapes=[
            pltpu.VMEM((2, 4, 4, 8, 8, 128), F32),
            pltpu.VMEM((256, 128), F32),
            pltpu.VMEM((256, 128), F32),
            pltpu.VMEM((ORDER, ORDER), F32),
            pltpu.VMEM((ORDER, ORDER), F32),
            dma((3,)),
            dma((3,)),
            dma((8,)),
            dma((8,)),
            dma((15,)),
            dma((15,)),
            dma((16,)),
            dma((16,)),
            dma,
            dma,
            dma((9,)),
            dma((9,)),
            dma((8,)),
            dma((8,)),
            dma((2, 7)),
            dma((2, 7)),
            dma,
        ],
        compiler_params=pltpu.CompilerParams(collective_id=0, has_side_effects=True),
        name="exchange_and_factor",
    )(diag_block, panel)


def split2(x):
    high = x.astype(BF16)
    return high, (x - high.astype(F32)).astype(BF16)


def dot_nt(left, right):
    lh, ll = left
    rh, rl = right
    dims = (((1,), (1,)), ((), ()))
    dot = functools.partial(lax.dot_general, dimension_numbers=dims, preferred_element_type=F32)
    return dot(lh, rh) + dot(lh, rl) + dot(ll, rh)


TILE = 256


def update_kernel(
    cols_ref, rows_ref, inv_ref, slab_ref, trail_ref,
    slab_out, panel_out, schur_ref, ih_ref, il_ref, sh_ref, sl_ref,
):
    step = pl.program_id(0)

    def solve(pieces):
        whole = jnp.concatenate(pieces, axis=1)
        ph, pl_ = split2(whole)
        left = dot_nt((ph[:, :256], pl_[:, :256]), (ih_ref[:256, :256], il_ref[:256, :256]))
        right = dot_nt((ph, pl_), (ih_ref[256:, :], il_ref[256:, :]))
        return jnp.concatenate([left, right], axis=1)

    @pl.when(step == 0)
    def _():
        slab_out[...] = slab_ref[...]
        ih_ref[...], il_ref[...] = split2(inv_ref[...])
        for q in range(4):
            part = solve([
                jnp.concatenate([cols_ref[0, e, q], cols_ref[1, q, e]], axis=0) for e in range(4)
            ])
            sh, sl = split2(part)
            sh_ref[256 * q : 256 * q + 256, :] = sh
            sl_ref[256 * q : 256 * q + 256, :] = sl

            @pl.when(lax.axis_index("col") == q)
            def _():
                for e in range(4):

                    @pl.when(lax.axis_index("depth") == e)
                    def _():
                        panel_out[...] = part[:, 128 * e : 128 * e + 128]

    mine = split2(solve([rows_ref[4 * step + e] for e in range(4)]))
    schur_ref[...] = trail_ref[...] - dot_nt(mine, (sh_ref[...], sl_ref[...]))


def solve_and_update(cols, rows, inverse, slab, trailing):
    whole = lambda *shape: pl.BlockSpec(
        shape, lambda i: (0,) * len(shape), pipeline_mode=pl.Buffered(1)
    )
    tile = pl.BlockSpec((TILE, 1024), lambda i: (i, 0))
    return pl.pallas_call(
        update_kernel,
        grid_spec=pltpu.PrefetchScalarGridSpec(
            num_scalar_prefetch=0,
            grid=(1024 // TILE,),
            in_specs=[whole(2, 4, 4, 128, 128), whole(16, 256, 128), whole(ORDER, ORDER), whole(8, ORDER), tile],
            out_specs=(
                pl.BlockSpec((8, ORDER), lambda i: (0, 0)),
                pl.BlockSpec((256, 128), lambda i: (0, 0)),
                tile,
            ),
            scratch_shapes=[
                pltpu.VMEM((ORDER, ORDER), BF16),
                pltpu.VMEM((ORDER, ORDER), BF16),
                pltpu.VMEM((1024, ORDER), BF16),
                pltpu.VMEM((1024, ORDER), BF16),
            ],
        ),
        out_shape=(
            jax.ShapeDtypeStruct((8, ORDER), F32),
            jax.ShapeDtypeStruct((256, 128), F32),
            jax.ShapeDtypeStruct((1024, 1024), F32),
        ),
        name="solve_and_update",
    )(cols, rows, inverse, slab, trailing)


def local(diag_block, panel, trailing):
    cols, rows, inverse, slab = exchange_and_factor(diag_block, panel)
    return solve_and_update(cols, rows, inverse, slab, trailing)


def solution(mesh):
    in_specs = (P(("row", "col"), None), P(("row", "col"), "depth"), P(("col", "depth"), "row"))
    out_specs = (P(("row", "col"), None), P(("row", "col"), "depth"), P(("col", "depth"), "row"))
    return jax.shard_map(local, mesh=mesh, in_specs=in_specs, out_specs=out_specs, check_vma=False)
```

```python
import functools

import jax
import jax.numpy as jnp
from jax import lax
from jax.experimental import pallas as pl
from jax.experimental.pallas import tpu as pltpu
from jax.sharding import PartitionSpec as P

ORDER = 512
BAND = 32


def split3(x):
    high = x.astype(jnp.bfloat16)
    rest = x - high.astype(jnp.float32)
    mid = rest.astype(jnp.bfloat16)
    low = (rest - mid.astype(jnp.float32)).astype(jnp.bfloat16)
    return high, mid, low


def spread(rows, which):
    return jnp.broadcast_to(rows[which : which + 1, :], (8, 128))


def band_step(inv_ref, upper_ref, base, part):
    start = pl.multiple_of(base + BAND * part, BAND)
    group = pl.multiple_of(base, 128)
    tiles = BAND // 8
    here = inv_ref[pl.ds(start, BAND), pl.ds(group, 128)]
    lane = lax.broadcasted_iota(jnp.int32, (8, 128), 1)
    sub = lax.broadcasted_iota(jnp.int32, (8, 128), 0)
    cols = []
    for j in range(BAND):
        first = j // 8
        wide = jnp.broadcast_to(
            here[8 * first :, BAND * part + j : BAND * part + j + 1], (BAND - 8 * first, 128)
        )
        cols.append([None] * first + [wide[8 * t : 8 * t + 8] for t in range(tiles - first)])
    rows = []
    for q in range(4):
        strip = inv_ref[pl.ds(start, BAND), 128 * q : 128 * q + 128]
        rows.append([strip[8 * t : 8 * t + 8] for t in range(tiles)])
    rows.append(
        [jnp.where(lane == sub + (BAND * part + 8 * t), 1.0, 0.0) for t in range(tiles)]
    )
    for j in range(BAND):
        tj, sj = j // 8, j % 8
        scale = lax.rsqrt(spread(cols[j][tj], sj))
        factor = [None if col is None else col * scale for col in cols[j]]
        for k in range(j + 1, BAND):
            weight = spread(factor[k // 8], k % 8)
            for t in range(k // 8, tiles):
                cols[k][t] = cols[k][t] - factor[t] * weight
        below = jnp.where(sub > sj, factor[tj], 0.0)
        for strip in rows:
            row = spread(strip[tj], sj) * scale
            strip[tj] = jnp.where(sub == sj, row, strip[tj] - below * row)
            for t in range(tj + 1, tiles):
                strip[t] = strip[t] - factor[t] * row
    lanes = lax.broadcasted_iota(jnp.int32, (BAND, 128), 1)
    subs = lax.broadcasted_iota(jnp.int32, (BAND, 128), 0)
    solved = [jnp.concatenate(strip, axis=0) for strip in rows]
    right, whole = [], []
    for q in range(4):
        col = lanes + 128 * q
        upper_ref[pl.ds(start, BAND), 128 * q : 128 * q + 128] = jnp.where(
            col >= subs + start, solved[q], 0.0
        )
        right.append(jnp.where(col >= start + BAND, solved[q], 0.0))
        whole.append(jnp.where((col >= start) & (col < start + BAND), solved[4], solved[q]))
    right, whole = jnp.concatenate(right, axis=1), jnp.concatenate(whole, axis=1)
    uh, um, ul = split3(right)
    wh, wm, wl = split3(whole)
    product = lax.dot_general(
        jnp.concatenate([uh, uh, uh, um, um, ul, um, ul], axis=0),
        jnp.concatenate([wh, wm, wl, wh, wm, wh, wl, wm], axis=0),
        (((0,), (0,)), ((), ())),
        preferred_element_type=jnp.float32,
    )
    col = lax.broadcasted_iota(jnp.int32, (ORDER, ORDER), 1)
    inv_ref[...] = jnp.where((col >= start) & (col < start + BAND), 0.0, inv_ref[...]) - product
    inv_ref[pl.ds(start, BAND), :] = whole


MESH = pl.DeviceIdType.MESH
F32 = jnp.float32
BF16 = jnp.bfloat16
SHIFTS = sorted(
    [(i, j) for i in range(4) for j in range(4) if i or j],
    key=lambda s: -(min(s[0], 4 - s[0]) + min(s[1], 4 - s[1])),
)

FAR_FIRST = (4, 3, 5, 2, 6, 1, 7)


def exchange_kernel(
    diag_ref,
    panel_ref,
    cols_ref,
    rows_ref,
    inv_out,
    slab_ref,
    gathered,
    piece,
    turned,
    inv_ref,
    upper_ref,
    local_sem,
    keep_sem,
    z_send,
    z_recv,
    xy_send,
    xy_recv,
    pair_send,
    pair_recv,
    turn_send,
    turn_recv,
    rz_send,
    rz_recv,
    rp_send,
    rp_recv,
    c_send,
    c_recv,
    out_sem,
):
    row, c, d = lax.axis_index("row"), lax.axis_index("col"), lax.axis_index("depth")
    z, k = row // 2, row % 2
    block = 4 * c + d
    turn_c, turn_d = row // 4, row % 4
    fixed = block == row

    def at(row_id, col_id, depth_id):
        return {"row": row_id, "col": col_id, "depth": depth_id}

    def remote(src, dst, send, recv, where):
        return pltpu.make_async_remote_copy(
            src_ref=src, dst_ref=dst, send_sem=send, recv_sem=recv,
            device_id=where, device_id_type=MESH,
        )

    lane = pl.multiple_of(d * 128, 128)
    load_diag = pltpu.make_async_copy(
        diag_ref.at[:, pl.ds(lane, 128)], gathered.at[k, c, d, z], local_sem.at[0]
    )
    load_diag.start()
    load_piece = pltpu.make_async_copy(panel_ref, piece, local_sem.at[1])
    load_piece.start()

    @pl.when(fixed)
    def _():
        pltpu.make_async_copy(panel_ref, turned, local_sem.at[2]).start()

    barrier = pltpu.get_barrier_semaphore()

    def greet(where):
        pl.semaphore_signal(barrier, inc=1, device_id=where, device_id_type=MESH)

    z_peers = [at(2 * ((z + s) % 8) + k, c, d) for s in range(8)]
    xy_peers = [at(row, (c + i) % 4, (d + j) % 4) for i, j in SHIFTS]
    x_peers = [at(row, (c + i) % 4, d) for i in range(4)]
    y_peers = [at(row, c, (d + j) % 4) for j in range(4)]
    partner = at(2 * z + 1 - k, c, d)
    turn_peer = at(block, turn_c, turn_d)
    for s in FAR_FIRST:
        greet(z_peers[s])
    for peer in xy_peers:
        greet(peer)
    greet(partner)

    @pl.when(jnp.logical_not(fixed))
    def _():
        greet(turn_peer)

    @pl.when(fixed)
    def _():
        pl.semaphore_wait(barrier, 23)

    @pl.when(jnp.logical_not(fixed))
    def _():
        pl.semaphore_wait(barrier, 24)

    load_diag.wait()
    sent = []

    def start(copy):
        copy.start()
        sent.append(copy)

    for s in FAR_FIRST:
        start(remote(
            gathered.at[k, c, d, z], gathered.at[k, c, d, z], z_send.at[s], z_recv.at[s], z_peers[s]
        ))

    load_piece.wait()

    @pl.when(jnp.logical_not(fixed))
    def _():
        remote(piece, turned, turn_send, turn_recv, turn_peer).start()

    halves = [piece.at[:128], piece.at[128:]]
    own_slots = [cols_ref.at[0, d, c], cols_ref.at[1, c, d]]
    keeps = [pltpu.make_async_copy(halves[h], own_slots[h], keep_sem.at[h]) for h in range(2)]
    for h in range(2):
        for s in (2, 1, 3):
            peer = (x_peers, y_peers)[h][s]
            start(remote(halves[h], own_slots[h], c_send.at[h, s], c_recv.at[h, s], peer))
        keeps[h].start()

    for s in range(1, 8):
        from_z = (z - s + 8) % 8
        remote(
            gathered.at[k, c, d, from_z], gathered.at[k, c, d, from_z],
            z_send.at[s], z_recv.at[s], z_peers[s],
        ).wait_recv()

    for n in range(15):
        start(remote(
            gathered.at[k, c, d], gathered.at[k, c, d], xy_send.at[n], xy_recv.at[n], xy_peers[n]
        ))
    start(remote(
        gathered.at[k, c, d], gathered.at[k, c, d], pair_send.at[15], pair_recv.at[15], partner
    ))

    @pl.when(fixed)
    def _():
        pltpu.make_async_copy(panel_ref, turned, local_sem.at[2]).wait()

    @pl.when(jnp.logical_not(fixed))
    def _():
        remote(piece, turned, turn_send, turn_recv, turn_peer).wait_recv()

    for s in (2, 6, 1, 7):
        start(remote(turned, rows_ref.at[row], rz_send.at[s], rz_recv.at[s], z_peers[s]))
    keep_turned = pltpu.make_async_copy(turned, rows_ref.at[row], keep_sem.at[2])
    keep_turned.start()
    start(remote(turned, rows_ref.at[row], rp_send.at[0], rp_recv.at[0], partner))

    for n in reversed(range(15)):
        i, j = SHIFTS[n]
        fc, fd = (c - i + 4) % 4, (d - j + 4) % 4
        remote(
            gathered.at[k, fc, fd], gathered.at[k, fc, fd], xy_send.at[n], xy_recv.at[n], xy_peers[n]
        ).wait_recv()
        start(remote(
            gathered.at[k, fc, fd], gathered.at[k, fc, fd], pair_send.at[n], pair_recv.at[n], partner
        ))
    for n in reversed(range(16)):
        i, j = (0, 0) if n == 15 else SHIFTS[n]
        fc, fd = (c - i + 4) % 4, (d - j + 4) % 4
        remote(
            gathered.at[1 - k, fc, fd], gathered.at[1 - k, fc, fd],
            pair_send.at[n], pair_recv.at[n], partner,
        ).wait_recv()

    def half_from(h, s):
        if h == 0:
            return cols_ref.at[0, d, (c - s + 4) % 4]
        return cols_ref.at[1, c, (d - s + 4) % 4]

    for h in range(2):
        keeps[h].wait()
        for s in range(1, 4):
            slot = half_from(h, s)
            remote(slot, slot, c_send.at[h, s], c_recv.at[h, s], partner).wait_recv()
        line = cols_ref.at[h, (d, c)[h]]
        for s in (2, 1, 3):
            peer = (y_peers, x_peers)[h][s]
            start(remote(line, line, c_send.at[h, 3 + s], c_recv.at[h, 3 + s], peer))

    def from_row(s):
        return 2 * ((z - s + 8) % 8) + k

    def arrive(s):
        slot = rows_ref.at[from_row(s)]
        remote(slot, slot, rz_send.at[s], rz_recv.at[s], partner).wait_recv()

    def onward(s):
        slot = rows_ref.at[from_row(s)]
        return remote(slot, slot, rp_send.at[s], rp_recv.at[s], partner)

    def near_rows_on(act):
        for s, side in ((2, 0), (6, 1)):
            slot = rows_ref.at[from_row(s)]
            part = rows_ref.at[from_row(s), pl.ds(128 * side, 128)]
            ahead, twice = ((1, 2), (7, 6))[side]
            act(
                s,
                remote(part, part, rz_send.at[4 + 4 * side], rz_recv.at[4 + 4 * side], z_peers[twice]),
                remote(slot, slot, rz_send.at[3 + 2 * side], rz_recv.at[3 + 2 * side], z_peers[ahead]),
                onward(s),
            )
        for s in (1, 7):
            act(s, onward(s))

    def go_on(s, *copies):
        arrive(s)
        for copy in copies:
            copy.start()

    for fk in range(2):
        for fc in range(4):
            for fd in range(4):
                for fz in range(8):
                    first = (2 * fz + fk) * 32 + fc * 8
                    inv_ref[first : first + 8, 128 * fd : 128 * fd + 128] = gathered[fk, fc, fd, fz]

    @pl.loop(0, ORDER // 128)
    def _(step):
        @pl.when(step == 1)
        def _():
            near_rows_on(go_on)

        @pl.when(step == ORDER // 128 - 1)
        def _():
            for s in (3, 5):
                arrive(s)
                onward(s).start()
            for side in range(2):
                part = rows_ref.at[from_row(4), pl.ds(128 * side, 128)]
                sem = 4 + 4 * side
                remote(part, part, rz_send.at[sem], rz_recv.at[sem], partner).wait_recv()
            onward(4).start()

        for part in range(128 // BAND):
            band_step(inv_ref, upper_ref, step * 128, part)

    store_inv = pltpu.make_async_copy(inv_ref, inv_out, out_sem)
    store_inv.start()
    near_rows_on(lambda s, *copies: sent.extend(copies))
    for s in (3, 5, 4):
        sent.append(onward(s))

    mine = row * 4 + c
    group = pl.multiple_of((mine // 16) * 128, 128)
    upper_ref[:128, :] = upper_ref[:, pl.ds(group, 128)].T
    slab_ref[...] = upper_ref[pl.ds(pl.multiple_of((mine % 16) * 8, 8), 8), :]

    for h in range(2):
        for s in range(1, 4):
            line = cols_ref.at[h, ((d, c)[h] - s + 4) % 4]
            remote(line, line, c_send.at[h, 3 + s], c_recv.at[h, 3 + s], partner).wait_recv()
    for s in range(8):
        slot = rows_ref.at[2 * ((z - s + 8) % 8) + 1 - k]
        remote(slot, slot, rp_send.at[s], rp_recv.at[s], partner).wait_recv()

    @pl.when(jnp.logical_not(fixed))
    def _():
        remote(piece, turned, turn_send, turn_recv, turn_peer).wait_send()

    for copy in sent:
        copy.wait_send()
    keep_turned.wait()
    store_inv.wait()


def exchange_and_factor(diag_block, panel):
    hbm = pl.BlockSpec(memory_space=pltpu.MemorySpace.HBM)
    dma = pltpu.SemaphoreType.DMA
    return pl.pallas_call(
        exchange_kernel,
        out_shape=(
            jax.ShapeDtypeStruct((2, 4, 4, 128, 128), F32),
            jax.ShapeDtypeStruct((16, 256, 128), F32),
            jax.ShapeDtypeStruct((ORDER, ORDER), F32),
            jax.ShapeDtypeStruct((8, ORDER), F32),
        ),
        in_specs=[hbm, hbm],
        out_specs=(hbm, hbm, hbm, pl.BlockSpec(memory_space=pltpu.VMEM)),
        scratch_shapes=[
            pltpu.VMEM((2, 4, 4, 8, 8, 128), F32),
            pltpu.VMEM((256, 128), F32),
            pltpu.VMEM((256, 128), F32),
            pltpu.VMEM((ORDER, ORDER), F32),
            pltpu.VMEM((ORDER, ORDER), F32),
            dma((3,)),
            dma((3,)),
            dma((8,)),
            dma((8,)),
            dma((15,)),
            dma((15,)),
            dma((16,)),
            dma((16,)),
            dma,
            dma,
            dma((9,)),
            dma((9,)),
            dma((8,)),
            dma((8,)),
            dma((2, 7)),
            dma((2, 7)),
            dma,
        ],
        compiler_params=pltpu.CompilerParams(collective_id=0, has_side_effects=True),
        name="exchange_and_factor",
    )(diag_block, panel)


def split2(x):
    high = x.astype(BF16)
    return high, (x - high.astype(F32)).astype(BF16)


def dot3(left, right, depth_axis):
    (lh, ll), (rh, rl) = left, right
    return lax.dot_general(
        jnp.concatenate([lh, lh, ll], axis=1),
        jnp.concatenate([rh, rl, rh], axis=depth_axis),
        (((1,), (depth_axis,)), ((), ())),
        preferred_element_type=F32,
    )


def update_kernel(
    cols_ref, rows_ref, inv_ref, slab_ref, trail_ref,
    slab_out, panel_out, schur_ref, ih_ref, il_ref, sh_ref, sl_ref,
):
    def cols_piece(q):
        return split2(jnp.concatenate([
            jnp.concatenate([cols_ref[0, e, q], cols_ref[1, q, e]], axis=0) for e in range(4)
        ], axis=1))

    @pl.when(pl.program_id(0) == 0)
    def _():
        slab_out[...] = slab_ref[...]
        ih, il = split2(inv_ref[...])
        for q in range(4):
            ph, pl_ = cols_piece(q)
            top = dot3((ih[:256, :256], il[:256, :256]), (ph[:, :256], pl_[:, :256]), 1)
            low = dot3((ih[256:], il[256:]), (ph, pl_), 1)
            part = slice(256 * q, 256 * q + 256)
            sh_ref[:, part], sl_ref[:, part] = split2(jnp.concatenate([top, low], axis=0))
        ih_ref[...], il_ref[...] = split2(inv_ref[...].T)
        first = pl.multiple_of(lax.axis_index("depth") * 128, 128)
        panel_out[...] = dot3(
            cols_piece(lax.axis_index("col")), split2(inv_ref[pl.ds(first, 128), :]), 1
        )

    ph, pl_ = split2(jnp.concatenate([rows_ref[0, e] for e in range(4)], axis=1))
    left = dot3((ph[:, :256], pl_[:, :256]), (ih_ref[:256, :256], il_ref[:256, :256]), 0)
    right = dot3((ph, pl_), (ih_ref[:, 256:], il_ref[:, 256:]), 0)
    mine = split2(jnp.concatenate([left, right], axis=1))
    schur_ref[...] = trail_ref[...] - dot3(mine, (sh_ref[...], sl_ref[...]), 0)


TILE = 256


def solve_and_update(cols, rows, inverse, slab, trailing):
    def whole(*shape):
        return pl.BlockSpec(shape, lambda i: (0,) * len(shape), pipeline_mode=pl.Buffered(1))

    tile = pl.BlockSpec((TILE, 1024), lambda i: (i, 0))
    return pl.pallas_call(
        update_kernel,
        grid=(1024 // TILE,),
        in_specs=[
            whole(2, 4, 4, 128, 128),
            pl.BlockSpec((1, 4, TILE, 128), lambda i: (i, 0, 0, 0)),
            whole(ORDER, ORDER),
            whole(8, ORDER),
            tile,
        ],
        out_specs=(whole(8, ORDER), whole(256, 128), tile),
        out_shape=(
            jax.ShapeDtypeStruct((8, ORDER), F32),
            jax.ShapeDtypeStruct((256, 128), F32),
            jax.ShapeDtypeStruct((1024, 1024), F32),
        ),
        scratch_shapes=[
            pltpu.VMEM((ORDER, ORDER), BF16),
            pltpu.VMEM((ORDER, ORDER), BF16),
            pltpu.VMEM((ORDER, 1024), BF16),
            pltpu.VMEM((ORDER, 1024), BF16),
        ],
        name="solve_and_update",
    )(cols, rows.reshape(4, 4, TILE, 128), inverse, slab, trailing)


def local(diag_block, panel, trailing):
    cols, rows, inverse, slab = exchange_and_factor(diag_block, panel)
    return solve_and_update(cols, rows, inverse, slab, trailing)


def solution(mesh):
    in_specs = (P(("row", "col"), None), P(("row", "col"), "depth"), P(("col", "depth"), "row"))
    out_specs = (P(("row", "col"), None), P(("row", "col"), "depth"), P(("col", "depth"), "row"))
    return jax.shard_map(local, mesh=mesh, in_specs=in_specs, out_specs=out_specs, check_vma=False)
```

```python
import functools

import jax
import jax.numpy as jnp
from jax import lax
from jax.experimental import pallas as pl
from jax.experimental.pallas import tpu as pltpu
from jax.sharding import PartitionSpec as P

ORDER = 512
BAND = 32
F32 = jnp.float32
BF16 = jnp.bfloat16


def split3(x):
    high = x.astype(BF16)
    rest = x - high.astype(F32)
    mid = rest.astype(BF16)
    low = (rest - mid.astype(F32)).astype(BF16)
    return high, mid, low


def left_parts(x):
    h, m, l = split3(x)
    return jnp.concatenate([h, h, h, m, m, l], axis=0)


def right_parts(x):
    h, m, l = split3(x)
    return jnp.concatenate([h, m, l, h, m, h], axis=0)


def dot_tn(left, right):
    return lax.dot_general(left, right, (((0,), (0,)), ((), ())), preferred_element_type=F32)


def spread(rows, which):
    return jnp.broadcast_to(rows[which : which + 1, :], (8, 128))


def band_step(inv_ref, upper_ref, step, part):
    base = step * 128
    start = pl.multiple_of(base + BAND * part, BAND)
    group = pl.multiple_of(base, 128)
    tiles = BAND // 8
    here = inv_ref[pl.ds(start, BAND), pl.ds(group, 128)]
    lane = lax.broadcasted_iota(jnp.int32, (8, 128), 1)
    sub = lax.broadcasted_iota(jnp.int32, (8, 128), 0)
    cols = []
    for j in range(BAND):
        first = j // 8
        wide = jnp.broadcast_to(
            here[8 * first :, BAND * part + j : BAND * part + j + 1], (BAND - 8 * first, 128)
        )
        cols.append([None] * first + [wide[8 * t : 8 * t + 8] for t in range(tiles - first)])
    rows = []
    for q in range(4):
        strip = inv_ref[pl.ds(start, BAND), 128 * q : 128 * q + 128]
        rows.append([strip[8 * t : 8 * t + 8] for t in range(tiles)])
    rows.append(
        [jnp.where(lane == sub + (BAND * part + 8 * t), 1.0, 0.0) for t in range(tiles)]
    )
    for j in range(BAND):
        tj, sj = j // 8, j % 8
        scale = lax.rsqrt(spread(cols[j][tj], sj))
        factor = [None if col is None else col * scale for col in cols[j]]
        for k in range(j + 1, BAND):
            weight = spread(factor[k // 8], k % 8)
            for t in range(k // 8, tiles):
                cols[k][t] = cols[k][t] - factor[t] * weight
        below = jnp.where(sub > sj, factor[tj], 0.0)
        for strip in rows:
            row = spread(strip[tj], sj) * scale
            strip[tj] = jnp.where(sub == sj, row, strip[tj] - below * row)
            for t in range(tj + 1, tiles):
                strip[t] = strip[t] - factor[t] * row
    lanes = lax.broadcasted_iota(jnp.int32, (BAND, 128), 1)
    subs = lax.broadcasted_iota(jnp.int32, (BAND, 128), 0)
    solved = [jnp.concatenate(strip, axis=0) for strip in rows]
    near = solved[0]
    whole = []
    for q in range(4):
        col = lanes + 128 * q
        upper_ref[pl.ds(start, BAND), 128 * q : 128 * q + 128] = jnp.where(
            col >= subs + start, solved[q], 0.0
        )
        whole.append(jnp.where((col >= start) & (col < start + BAND), solved[4], solved[q]))
        if q:
            near = jnp.where(step == q, solved[q], near)
    whole = jnp.concatenate(whole, axis=1)
    inv_ref[pl.ds(start, BAND), :] = whole
    rest = 128 - BAND * (part + 1)
    if rest:
        product = dot_tn(left_parts(near), right_parts(whole))
        after = pl.multiple_of(start + BAND, BAND)
        col = lax.broadcasted_iota(jnp.int32, (rest, ORDER), 1)
        inv_ref[pl.ds(after, rest), :] = (
            jnp.where((col >= start) & (col < start + BAND), 0.0, inv_ref[pl.ds(after, rest), :])
            - product[128 - rest :, :]
        )


def group_step(inv_ref, upper_ref, parts_ref, step):
    first = pl.multiple_of(step * 128, 128)
    mine = inv_ref[pl.ds(first, 128), :]
    col = lax.broadcasted_iota(jnp.int32, (128, ORDER), 1)
    below = col <= lax.broadcasted_iota(jnp.int32, (128, ORDER), 0) + first
    parts_ref[...] = right_parts(jnp.where(below | (col >= first + 128), mine, 0.0))
    inv_ref[pl.ds(first, 128), :] = jnp.where(below, mine, 0.0)

    @pl.loop(step + 1, 4)
    def _(other):
        at = pl.multiple_of(other * 128, 128)
        product = dot_tn(
            left_parts(upper_ref[pl.ds(first, 128), pl.ds(at, 128)]), parts_ref[...]
        )
        inv_ref[pl.ds(at, 128), :] = (
            jnp.where((col >= first) & (col < first + 128), 0.0, inv_ref[pl.ds(at, 128), :])
            - product
        )


MESH = pl.DeviceIdType.MESH
SHIFTS = sorted(
    [(i, j) for i in range(4) for j in range(4) if i or j],
    key=lambda s: -(min(s[0], 4 - s[0]) + min(s[1], 4 - s[1])),
)

FAR_FIRST = (4, 3, 5, 2, 6, 1, 7)


def exchange_kernel(
    diag_ref,
    panel_ref,
    cols_ref,
    rows_ref,
    inv_out,
    slab_ref,
    gathered,
    piece,
    turned,
    inv_ref,
    upper_ref,
    parts_ref,
    local_sem,
    keep_sem,
    z_send,
    z_recv,
    xy_send,
    xy_recv,
    pair_send,
    pair_recv,
    turn_send,
    turn_recv,
    rz_send,
    rz_recv,
    rp_send,
    rp_recv,
    c_send,
    c_recv,
    out_sem,
):
    row, c, d = lax.axis_index("row"), lax.axis_index("col"), lax.axis_index("depth")
    z, k = row // 2, row % 2
    block = 4 * c + d
    turn_c, turn_d = row // 4, row % 4
    fixed = block == row

    def at(row_id, col_id, depth_id):
        return {"row": row_id, "col": col_id, "depth": depth_id}

    def remote(src, dst, send, recv, where):
        return pltpu.make_async_remote_copy(
            src_ref=src, dst_ref=dst, send_sem=send, recv_sem=recv,
            device_id=where, device_id_type=MESH,
        )

    lane = pl.multiple_of(d * 128, 128)
    load_diag = pltpu.make_async_copy(
        diag_ref.at[:, pl.ds(lane, 128)], gathered.at[k, c, d, z], local_sem.at[0]
    )
    load_diag.start()
    load_piece = pltpu.make_async_copy(panel_ref, piece, local_sem.at[1])
    load_piece.start()

    @pl.when(fixed)
    def _():
        pltpu.make_async_copy(panel_ref, turned, local_sem.at[2]).start()

    barrier = pltpu.get_barrier_semaphore()

    def greet(where):
        pl.semaphore_signal(barrier, inc=1, device_id=where, device_id_type=MESH)

    z_peers = [at(2 * ((z + s) % 8) + k, c, d) for s in range(8)]
    xy_peers = [at(row, (c + i) % 4, (d + j) % 4) for i, j in SHIFTS]
    x_peers = [at(row, (c + i) % 4, d) for i in range(4)]
    y_peers = [at(row, c, (d + j) % 4) for j in range(4)]
    partner = at(2 * z + 1 - k, c, d)
    turn_peer = at(block, turn_c, turn_d)
    for s in FAR_FIRST:
        greet(z_peers[s])
    for peer in xy_peers:
        greet(peer)
    greet(partner)

    @pl.when(jnp.logical_not(fixed))
    def _():
        greet(turn_peer)

    @pl.when(fixed)
    def _():
        pl.semaphore_wait(barrier, 23)

    @pl.when(jnp.logical_not(fixed))
    def _():
        pl.semaphore_wait(barrier, 24)

    load_diag.wait()
    sent = []

    def start(copy):
        copy.start()
        sent.append(copy)

    for s in FAR_FIRST:
        start(remote(
            gathered.at[k, c, d, z], gathered.at[k, c, d, z], z_send.at[s], z_recv.at[s], z_peers[s]
        ))

    load_piece.wait()

    @pl.when(jnp.logical_not(fixed))
    def _():
        remote(piece, turned, turn_send, turn_recv, turn_peer).start()

    halves = [piece.at[:128], piece.at[128:]]
    own_slots = [cols_ref.at[0, d, c], cols_ref.at[1, c, d]]
    keeps = [pltpu.make_async_copy(halves[h], own_slots[h], keep_sem.at[h]) for h in range(2)]
    for h in range(2):
        for s in (2, 1, 3):
            peer = (x_peers, y_peers)[h][s]
            start(remote(halves[h], own_slots[h], c_send.at[h, s], c_recv.at[h, s], peer))
        keeps[h].start()

    for s in range(1, 8):
        from_z = (z - s + 8) % 8
        remote(
            gathered.at[k, c, d, from_z], gathered.at[k, c, d, from_z],
            z_send.at[s], z_recv.at[s], z_peers[s],
        ).wait_recv()

    early, late = pl.ds(0, 2), pl.ds(2, 6)

    def across(n, part):
        slot = gathered.at[k, c, d, (early, late)[part]]
        return remote(slot, slot, xy_send.at[part, n], xy_recv.at[part, n], xy_peers[n])

    def origin(n):
        i, j = (0, 0) if n == 15 else SHIFTS[n]
        return (c - i + 4) % 4, (d - j + 4) % 4

    def crossed(n, part):
        fc, fd = origin(n)
        slot = gathered.at[k, fc, fd, (early, late)[part]]
        remote(slot, slot, xy_send.at[part, n], xy_recv.at[part, n], partner).wait_recv()

    def to_pair(n, part):
        fc, fd = origin(n)
        slot = gathered.at[k, fc, fd, (early, late)[part]]
        return remote(slot, slot, pair_send.at[part, n], pair_recv.at[part, n], partner)

    def from_pair(n, part):
        fc, fd = origin(n)
        slot = gathered.at[1 - k, fc, fd, (early, late)[part]]
        remote(slot, slot, pair_send.at[part, n], pair_recv.at[part, n], partner).wait_recv()

    for part in range(2):
        for n in range(15):
            start(across(n, part))
        start(to_pair(15, part))

    @pl.when(fixed)
    def _():
        pltpu.make_async_copy(panel_ref, turned, local_sem.at[2]).wait()

    @pl.when(jnp.logical_not(fixed))
    def _():
        remote(piece, turned, turn_send, turn_recv, turn_peer).wait_recv()

    for s in (2, 6, 1, 7):
        start(remote(turned, rows_ref.at[row], rz_send.at[s], rz_recv.at[s], z_peers[s]))
    keep_turned = pltpu.make_async_copy(turned, rows_ref.at[row], keep_sem.at[2])
    keep_turned.start()
    start(remote(turned, rows_ref.at[row], rp_send.at[0], rp_recv.at[0], partner))

    for n in reversed(range(15)):
        crossed(n, 0)
        start(to_pair(n, 0))
    for n in reversed(range(16)):
        from_pair(n, 0)

    def half_from(h, s):
        if h == 0:
            return cols_ref.at[0, d, (c - s + 4) % 4]
        return cols_ref.at[1, c, (d - s + 4) % 4]

    for h in range(2):
        keeps[h].wait()
        for s in range(1, 4):
            slot = half_from(h, s)
            remote(slot, slot, c_send.at[h, s], c_recv.at[h, s], partner).wait_recv()
        line = cols_ref.at[h, (d, c)[h]]
        for s in (2, 1, 3):
            peer = (y_peers, x_peers)[h][s]
            start(remote(line, line, c_send.at[h, 3 + s], c_recv.at[h, 3 + s], peer))

    def from_row(s):
        return 2 * ((z - s + 8) % 8) + k

    def arrive(s):
        slot = rows_ref.at[from_row(s)]
        remote(slot, slot, rz_send.at[s], rz_recv.at[s], partner).wait_recv()

    def onward(s):
        slot = rows_ref.at[from_row(s)]
        return remote(slot, slot, rp_send.at[s], rp_recv.at[s], partner)

    def near_rows_on(act):
        for s, side in ((2, 0), (6, 1)):
            slot = rows_ref.at[from_row(s)]
            part = rows_ref.at[from_row(s), pl.ds(128 * side, 128)]
            ahead, twice = ((1, 2), (7, 6))[side]
            act(
                s,
                remote(part, part, rz_send.at[4 + 4 * side], rz_recv.at[4 + 4 * side], z_peers[twice]),
                remote(slot, slot, rz_send.at[3 + 2 * side], rz_recv.at[3 + 2 * side], z_peers[ahead]),
                onward(s),
            )
        for s in (1, 7):
            act(s, onward(s))

    def go_on(s, *copies):
        arrive(s)
        for copy in copies:
            copy.start()

    def lay_out(planes):
        for fk in range(2):
            for fc in range(4):
                for fd in range(4):
                    for fz in planes:
                        first = (2 * fz + fk) * 32 + fc * 8
                        inv_ref[first : first + 8, 128 * fd : 128 * fd + 128] = gathered[fk, fc, fd, fz]

    lay_out(range(2))

    def store_group(step):
        part = pl.ds(pl.multiple_of(step * 128, 128), 128)
        return pltpu.make_async_copy(inv_ref.at[part], inv_out.at[part], out_sem.at[step])

    @pl.loop(0, ORDER // 128)
    def _(step):
        @pl.when(step == 1)
        def _():
            near_rows_on(go_on)

        @pl.when(step == ORDER // 128 - 1)
        def _():
            for s in (3, 5):
                arrive(s)
                onward(s).start()
            for side in range(2):
                part = rows_ref.at[from_row(4), pl.ds(128 * side, 128)]
                sem = 4 + 4 * side
                remote(part, part, rz_send.at[sem], rz_recv.at[sem], partner).wait_recv()
            onward(4).start()

        for part in range(128 // BAND):
            band_step(inv_ref, upper_ref, step, part)
            if part == 1:

                @pl.when(step == 0)
                def _():
                    for n in reversed(range(15)):
                        crossed(n, 1)
                        to_pair(n, 1).start()

        @pl.when(step == 0)
        def _():
            for n in reversed(range(16)):
                from_pair(n, 1)
            lay_out(range(2, 8))

        group_step(inv_ref, upper_ref, parts_ref, step)
        store_group(step).start()

    sent.extend(to_pair(n, 1) for n in range(15))
    near_rows_on(lambda s, *copies: sent.extend(copies))
    for s in (3, 5, 4):
        sent.append(onward(s))

    mine = row * 4 + c
    group = pl.multiple_of((mine // 16) * 128, 128)
    upper_ref[:128, :] = upper_ref[:, pl.ds(group, 128)].T
    slab_ref[...] = upper_ref[pl.ds(pl.multiple_of((mine % 16) * 8, 8), 8), :]

    for h in range(2):
        for s in range(1, 4):
            line = cols_ref.at[h, ((d, c)[h] - s + 4) % 4]
            remote(line, line, c_send.at[h, 3 + s], c_recv.at[h, 3 + s], partner).wait_recv()
    for s in range(8):
        slot = rows_ref.at[2 * ((z - s + 8) % 8) + 1 - k]
        remote(slot, slot, rp_send.at[s], rp_recv.at[s], partner).wait_recv()

    @pl.when(jnp.logical_not(fixed))
    def _():
        remote(piece, turned, turn_send, turn_recv, turn_peer).wait_send()

    for copy in sent:
        copy.wait_send()
    keep_turned.wait()
    for step in range(ORDER // 128):
        store_group(step).wait()


def exchange_and_factor(diag_block, panel):
    hbm = pl.BlockSpec(memory_space=pltpu.MemorySpace.HBM)
    dma = pltpu.SemaphoreType.DMA
    return pl.pallas_call(
        exchange_kernel,
        out_shape=(
            jax.ShapeDtypeStruct((2, 4, 4, 128, 128), F32),
            jax.ShapeDtypeStruct((16, 256, 128), F32),
            jax.ShapeDtypeStruct((ORDER, ORDER), F32),
            jax.ShapeDtypeStruct((8, ORDER), F32),
        ),
        in_specs=[hbm, hbm],
        out_specs=(hbm, hbm, hbm, pl.BlockSpec(memory_space=pltpu.VMEM)),
        scratch_shapes=[
            pltpu.VMEM((2, 4, 4, 8, 8, 128), F32),
            pltpu.VMEM((256, 128), F32),
            pltpu.VMEM((256, 128), F32),
            pltpu.VMEM((ORDER, ORDER), F32),
            pltpu.VMEM((ORDER, ORDER), F32),
            pltpu.VMEM((6 * 128, ORDER), BF16),
            dma((3,)),
            dma((3,)),
            dma((8,)),
            dma((8,)),
            dma((2, 15)),
            dma((2, 15)),
            dma((2, 16)),
            dma((2, 16)),
            dma,
            dma,
            dma((9,)),
            dma((9,)),
            dma((8,)),
            dma((8,)),
            dma((2, 7)),
            dma((2, 7)),
            dma((4,)),
        ],
        compiler_params=pltpu.CompilerParams(collective_id=0, has_side_effects=True),
        name="exchange_and_factor",
    )(diag_block, panel)


def split2(x):
    high = x.astype(BF16)
    return high, (x - high.astype(F32)).astype(BF16)


def dot3(left, right, depth_axis):
    (lh, ll), (rh, rl) = left, right
    return lax.dot_general(
        jnp.concatenate([lh, lh, ll], axis=1),
        jnp.concatenate([rh, rl, rh], axis=depth_axis),
        (((1,), (depth_axis,)), ((), ())),
        preferred_element_type=F32,
    )


def update_kernel(
    cols_ref, rows_ref, inv_ref, slab_ref, trail_ref,
    slab_out, panel_out, schur_ref, ih_ref, il_ref, sh_ref, sl_ref,
):
    def cols_piece(q):
        return split2(jnp.concatenate([
            jnp.concatenate([cols_ref[0, e, q], cols_ref[1, q, e]], axis=0) for e in range(4)
        ], axis=1))

    @pl.when(pl.program_id(0) == 0)
    def _():
        slab_out[...] = slab_ref[...]
        ih, il = split2(inv_ref[...])
        for q in range(4):
            ph, pl_ = cols_piece(q)
            top = dot3((ih[:256, :256], il[:256, :256]), (ph[:, :256], pl_[:, :256]), 1)
            low = dot3((ih[256:], il[256:]), (ph, pl_), 1)
            part = slice(256 * q, 256 * q + 256)
            sh_ref[:, part], sl_ref[:, part] = split2(jnp.concatenate([top, low], axis=0))
        ih_ref[...], il_ref[...] = split2(inv_ref[...].T)
        first = pl.multiple_of(lax.axis_index("depth") * 128, 128)
        panel_out[...] = dot3(
            cols_piece(lax.axis_index("col")), split2(inv_ref[pl.ds(first, 128), :]), 1
        )

    ph, pl_ = split2(jnp.concatenate([rows_ref[0, e] for e in range(4)], axis=1))
    left = dot3((ph[:, :256], pl_[:, :256]), (ih_ref[:256, :256], il_ref[:256, :256]), 0)
    right = dot3((ph, pl_), (ih_ref[:, 256:], il_ref[:, 256:]), 0)
    mine = split2(jnp.concatenate([left, right], axis=1))
    schur_ref[...] = trail_ref[...] - dot3(mine, (sh_ref[...], sl_ref[...]), 0)


TILE = 256


def solve_and_update(cols, rows, inverse, slab, trailing):
    def whole(*shape):
        return pl.BlockSpec(shape, lambda i: (0,) * len(shape), pipeline_mode=pl.Buffered(1))

    tile = pl.BlockSpec((TILE, 1024), lambda i: (i, 0))
    return pl.pallas_call(
        update_kernel,
        grid=(1024 // TILE,),
        in_specs=[
            whole(2, 4, 4, 128, 128),
            pl.BlockSpec((1, 4, TILE, 128), lambda i: (i, 0, 0, 0)),
            whole(ORDER, ORDER),
            whole(8, ORDER),
            tile,
        ],
        out_specs=(whole(8, ORDER), whole(256, 128), tile),
        out_shape=(
            jax.ShapeDtypeStruct((8, ORDER), F32),
            jax.ShapeDtypeStruct((256, 128), F32),
            jax.ShapeDtypeStruct((1024, 1024), F32),
        ),
        scratch_shapes=[
            pltpu.VMEM((ORDER, ORDER), BF16),
            pltpu.VMEM((ORDER, ORDER), BF16),
            pltpu.VMEM((ORDER, 1024), BF16),
            pltpu.VMEM((ORDER, 1024), BF16),
        ],
        name="solve_and_update",
    )(cols, rows.reshape(4, 4, TILE, 128), inverse, slab, trailing)


def local(diag_block, panel, trailing):
    cols, rows, inverse, slab = exchange_and_factor(diag_block, panel)
    return solve_and_update(cols, rows, inverse, slab, trailing)


def solution(mesh):
    in_specs = (P(("row", "col"), None), P(("row", "col"), "depth"), P(("col", "depth"), "row"))
    out_specs = (P(("row", "col"), None), P(("row", "col"), "depth"), P(("col", "depth"), "row"))
    return jax.shard_map(local, mesh=mesh, in_specs=in_specs, out_specs=out_specs, check_vma=False)
```

```python
import functools

import jax
import jax.numpy as jnp
from jax import lax
from jax.experimental import pallas as pl
from jax.experimental.pallas import tpu as pltpu
from jax.sharding import PartitionSpec as P

ORDER = 512
BAND = 32
F32 = jnp.float32
BF16 = jnp.bfloat16


def split3(x):
    high = x.astype(BF16)
    rest = x - high.astype(F32)
    mid = rest.astype(BF16)
    low = (rest - mid.astype(F32)).astype(BF16)
    return high, mid, low


def left_parts(x):
    h, m, l = split3(x)
    return jnp.concatenate([h, h, h, m, m, l], axis=0)


def right_parts(x):
    h, m, l = split3(x)
    return jnp.concatenate([h, m, l, h, m, h], axis=0)


def dot_tn(left, right):
    return lax.dot_general(left, right, (((0,), (0,)), ((), ())), preferred_element_type=F32)


def spread(rows, which):
    return jnp.broadcast_to(rows[which : which + 1, :], (8, 128))


def band_step(inv_ref, upper_ref, step, part):
    base = step * 128
    start = pl.multiple_of(base + BAND * part, BAND)
    group = pl.multiple_of(base, 128)
    tiles = BAND // 8
    here = inv_ref[pl.ds(start, BAND), pl.ds(group, 128)]
    lane = lax.broadcasted_iota(jnp.int32, (8, 128), 1)
    sub = lax.broadcasted_iota(jnp.int32, (8, 128), 0)
    cols = []
    for j in range(BAND):
        first = j // 8
        wide = jnp.broadcast_to(
            here[8 * first :, BAND * part + j : BAND * part + j + 1], (BAND - 8 * first, 128)
        )
        cols.append([None] * first + [wide[8 * t : 8 * t + 8] for t in range(tiles - first)])
    rows = []
    for q in range(4):
        strip = inv_ref[pl.ds(start, BAND), 128 * q : 128 * q + 128]
        rows.append([strip[8 * t : 8 * t + 8] for t in range(tiles)])
    rows.append(
        [jnp.where(lane == sub + (BAND * part + 8 * t), 1.0, 0.0) for t in range(tiles)]
    )
    for j in range(BAND):
        tj, sj = j // 8, j % 8
        scale = lax.rsqrt(spread(cols[j][tj], sj))
        factor = [None if col is None else col * scale for col in cols[j]]
        for k in range(j + 1, BAND):
            weight = spread(factor[k // 8], k % 8)
            for t in range(k // 8, tiles):
                cols[k][t] = cols[k][t] - factor[t] * weight
        below = jnp.where(sub > sj, factor[tj], 0.0)
        for strip in rows:
            row = spread(strip[tj], sj) * scale
            strip[tj] = jnp.where(sub == sj, row, strip[tj] - below * row)
            for t in range(tj + 1, tiles):
                strip[t] = strip[t] - factor[t] * row
    lanes = lax.broadcasted_iota(jnp.int32, (BAND, 128), 1)
    subs = lax.broadcasted_iota(jnp.int32, (BAND, 128), 0)
    solved = [jnp.concatenate(strip, axis=0) for strip in rows]
    near = solved[0]
    whole = []
    for q in range(4):
        col = lanes + 128 * q
        upper_ref[pl.ds(start, BAND), 128 * q : 128 * q + 128] = jnp.where(
            col >= subs + start, solved[q], 0.0
        )
        whole.append(jnp.where((col >= start) & (col < start + BAND), solved[4], solved[q]))
        if q:
            near = jnp.where(step == q, solved[q], near)
    whole = jnp.concatenate(whole, axis=1)
    inv_ref[pl.ds(start, BAND), :] = whole
    rest = 128 - BAND * (part + 1)
    if rest:
        product = dot_tn(left_parts(near), right_parts(whole))
        after = pl.multiple_of(start + BAND, BAND)
        col = lax.broadcasted_iota(jnp.int32, (rest, ORDER), 1)
        inv_ref[pl.ds(after, rest), :] = (
            jnp.where((col >= start) & (col < start + BAND), 0.0, inv_ref[pl.ds(after, rest), :])
            - product[128 - rest :, :]
        )


def group_step(inv_ref, upper_ref, parts_ref, step):
    first = pl.multiple_of(step * 128, 128)
    mine = inv_ref[pl.ds(first, 128), :]
    col = lax.broadcasted_iota(jnp.int32, (128, ORDER), 1)
    below = col <= lax.broadcasted_iota(jnp.int32, (128, ORDER), 0) + first
    parts_ref[...] = right_parts(jnp.where(below | (col >= first + 128), mine, 0.0))
    inv_ref[pl.ds(first, 128), :] = jnp.where(below, mine, 0.0)

    for done in range(1, 4):

        @pl.when(step == done - 1)
        def _():
            left = ORDER - 128 * done
            product = dot_tn(
                left_parts(upper_ref[128 * (done - 1) : 128 * done, 128 * done :]), parts_ref[...]
            )
            col = lax.broadcasted_iota(jnp.int32, (left, ORDER), 1)
            gone = (col >= 128 * (done - 1)) & (col < 128 * done)
            inv_ref[128 * done :, :] = jnp.where(gone, 0.0, inv_ref[128 * done :, :]) - product


MESH = pl.DeviceIdType.MESH
SHIFTS = sorted(
    [(i, j) for i in range(4) for j in range(4) if i or j],
    key=lambda s: -(min(s[0], 4 - s[0]) + min(s[1], 4 - s[1])),
)

FAR_FIRST = (4, 3, 5, 2, 6, 1, 7)


def exchange_kernel(
    diag_ref,
    panel_ref,
    cols_ref,
    rows_ref,
    inv_out,
    slab_ref,
    gathered,
    piece,
    turned,
    inv_ref,
    upper_ref,
    parts_ref,
    local_sem,
    keep_sem,
    z_send,
    z_recv,
    xy_send,
    xy_recv,
    pair_send,
    pair_recv,
    turn_send,
    turn_recv,
    rz_send,
    rz_recv,
    rp_send,
    rp_recv,
    c_send,
    c_recv,
    out_sem,
):
    row, c, d = lax.axis_index("row"), lax.axis_index("col"), lax.axis_index("depth")
    z, k = row // 2, row % 2
    block = 4 * c + d
    turn_c, turn_d = row // 4, row % 4
    fixed = block == row

    def at(row_id, col_id, depth_id):
        return {"row": row_id, "col": col_id, "depth": depth_id}

    def remote(src, dst, send, recv, where):
        return pltpu.make_async_remote_copy(
            src_ref=src, dst_ref=dst, send_sem=send, recv_sem=recv,
            device_id=where, device_id_type=MESH,
        )

    lane = pl.multiple_of(d * 128, 128)
    load_diag = pltpu.make_async_copy(
        diag_ref.at[:, pl.ds(lane, 128)], gathered.at[k, c, d, z], local_sem.at[0]
    )
    load_diag.start()
    load_piece = pltpu.make_async_copy(panel_ref, piece, local_sem.at[1])
    load_piece.start()

    @pl.when(fixed)
    def _():
        pltpu.make_async_copy(panel_ref, turned, local_sem.at[2]).start()

    barrier = pltpu.get_barrier_semaphore()

    def greet(where):
        pl.semaphore_signal(barrier, inc=1, device_id=where, device_id_type=MESH)

    z_peers = [at(2 * ((z + s) % 8) + k, c, d) for s in range(8)]
    xy_peers = [at(row, (c + i) % 4, (d + j) % 4) for i, j in SHIFTS]
    x_peers = [at(row, (c + i) % 4, d) for i in range(4)]
    y_peers = [at(row, c, (d + j) % 4) for j in range(4)]
    partner = at(2 * z + 1 - k, c, d)
    turn_peer = at(block, turn_c, turn_d)
    for s in FAR_FIRST:
        greet(z_peers[s])
    for peer in xy_peers:
        greet(peer)
    greet(partner)

    @pl.when(jnp.logical_not(fixed))
    def _():
        greet(turn_peer)

    @pl.when(fixed)
    def _():
        pl.semaphore_wait(barrier, 23)

    @pl.when(jnp.logical_not(fixed))
    def _():
        pl.semaphore_wait(barrier, 24)

    load_diag.wait()
    sent = []

    def start(copy):
        copy.start()
        sent.append(copy)

    for s in FAR_FIRST:
        start(remote(
            gathered.at[k, c, d, z], gathered.at[k, c, d, z], z_send.at[s], z_recv.at[s], z_peers[s]
        ))

    load_piece.wait()

    @pl.when(jnp.logical_not(fixed))
    def _():
        remote(piece, turned, turn_send, turn_recv, turn_peer).start()

    halves = [piece.at[:128], piece.at[128:]]
    own_slots = [cols_ref.at[0, d, c], cols_ref.at[1, c, d]]
    keeps = [pltpu.make_async_copy(halves[h], own_slots[h], keep_sem.at[h]) for h in range(2)]
    for h in range(2):
        for s in (2, 1, 3):
            peer = (x_peers, y_peers)[h][s]
            start(remote(halves[h], own_slots[h], c_send.at[h, s], c_recv.at[h, s], peer))
        keeps[h].start()

    for s in range(1, 8):
        from_z = (z - s + 8) % 8
        remote(
            gathered.at[k, c, d, from_z], gathered.at[k, c, d, from_z],
            z_send.at[s], z_recv.at[s], z_peers[s],
        ).wait_recv()

    early, late = pl.ds(0, 2), pl.ds(2, 6)

    def across(n, part):
        slot = gathered.at[k, c, d, (early, late)[part]]
        return remote(slot, slot, xy_send.at[part, n], xy_recv.at[part, n], xy_peers[n])

    def origin(n):
        i, j = (0, 0) if n == 15 else SHIFTS[n]
        return (c - i + 4) % 4, (d - j + 4) % 4

    def crossed(n, part):
        fc, fd = origin(n)
        slot = gathered.at[k, fc, fd, (early, late)[part]]
        remote(slot, slot, xy_send.at[part, n], xy_recv.at[part, n], partner).wait_recv()

    def to_pair(n, part):
        fc, fd = origin(n)
        slot = gathered.at[k, fc, fd, (early, late)[part]]
        return remote(slot, slot, pair_send.at[part, n], pair_recv.at[part, n], partner)

    def from_pair(n, part):
        fc, fd = origin(n)
        slot = gathered.at[1 - k, fc, fd, (early, late)[part]]
        remote(slot, slot, pair_send.at[part, n], pair_recv.at[part, n], partner).wait_recv()

    for part in range(2):
        for n in range(15):
            start(across(n, part))
        start(to_pair(15, part))

    @pl.when(fixed)
    def _():
        pltpu.make_async_copy(panel_ref, turned, local_sem.at[2]).wait()

    @pl.when(jnp.logical_not(fixed))
    def _():
        remote(piece, turned, turn_send, turn_recv, turn_peer).wait_recv()

    for s in (2, 6, 1, 7):
        start(remote(turned, rows_ref.at[row], rz_send.at[s], rz_recv.at[s], z_peers[s]))
    keep_turned = pltpu.make_async_copy(turned, rows_ref.at[row], keep_sem.at[2])
    keep_turned.start()
    start(remote(turned, rows_ref.at[row], rp_send.at[0], rp_recv.at[0], partner))

    for n in reversed(range(15)):
        crossed(n, 0)
        start(to_pair(n, 0))
    for n in reversed(range(16)):
        from_pair(n, 0)

    def half_from(h, s):
        if h == 0:
            return cols_ref.at[0, d, (c - s + 4) % 4]
        return cols_ref.at[1, c, (d - s + 4) % 4]

    for h in range(2):
        keeps[h].wait()
        for s in range(1, 4):
            slot = half_from(h, s)
            remote(slot, slot, c_send.at[h, s], c_recv.at[h, s], partner).wait_recv()
        line = cols_ref.at[h, (d, c)[h]]
        for s in (2, 1, 3):
            peer = (y_peers, x_peers)[h][s]
            start(remote(line, line, c_send.at[h, 3 + s], c_recv.at[h, 3 + s], peer))

    def from_row(s):
        return 2 * ((z - s + 8) % 8) + k

    def arrive(s):
        slot = rows_ref.at[from_row(s)]
        remote(slot, slot, rz_send.at[s], rz_recv.at[s], partner).wait_recv()

    def onward(s):
        slot = rows_ref.at[from_row(s)]
        return remote(slot, slot, rp_send.at[s], rp_recv.at[s], partner)

    def near_rows_on(act):
        for s, side in ((2, 0), (6, 1)):
            slot = rows_ref.at[from_row(s)]
            part = rows_ref.at[from_row(s), pl.ds(128 * side, 128)]
            ahead, twice = ((1, 2), (7, 6))[side]
            act(
                s,
                remote(part, part, rz_send.at[4 + 4 * side], rz_recv.at[4 + 4 * side], z_peers[twice]),
                remote(slot, slot, rz_send.at[3 + 2 * side], rz_recv.at[3 + 2 * side], z_peers[ahead]),
                onward(s),
            )
        for s in (1, 7):
            act(s, onward(s))

    def go_on(s, *copies):
        arrive(s)
        for copy in copies:
            copy.start()

    def lay_out(planes):
        for fk in range(2):
            for fc in range(4):
                for fd in range(4):
                    for fz in planes:
                        first = (2 * fz + fk) * 32 + fc * 8
                        inv_ref[first : first + 8, 128 * fd : 128 * fd + 128] = gathered[fk, fc, fd, fz]

    lay_out(range(2))

    def store_group(step):
        part = pl.ds(pl.multiple_of(step * 128, 128), 128)
        return pltpu.make_async_copy(inv_ref.at[part], inv_out.at[part], out_sem.at[step])

    @pl.loop(0, ORDER // 128)
    def _(step):
        @pl.when(step == 1)
        def _():
            near_rows_on(go_on)

        @pl.when(step == ORDER // 128 - 1)
        def _():
            for s in (3, 5):
                arrive(s)
                onward(s).start()
            for side in range(2):
                part = rows_ref.at[from_row(4), pl.ds(128 * side, 128)]
                sem = 4 + 4 * side
                remote(part, part, rz_send.at[sem], rz_recv.at[sem], partner).wait_recv()
            onward(4).start()

        for part in range(128 // BAND):
            band_step(inv_ref, upper_ref, step, part)
            if part == 1:

                @pl.when(step == 0)
                def _():
                    for n in reversed(range(15)):
                        crossed(n, 1)
                        to_pair(n, 1).start()

        @pl.when(step == 0)
        def _():
            for n in reversed(range(16)):
                from_pair(n, 1)
            lay_out(range(2, 8))

        group_step(inv_ref, upper_ref, parts_ref, step)
        store_group(step).start()

    sent.extend(to_pair(n, 1) for n in range(15))
    near_rows_on(lambda s, *copies: sent.extend(copies))
    for s in (3, 5, 4):
        sent.append(onward(s))

    mine = row * 4 + c
    group = pl.multiple_of((mine // 16) * 128, 128)
    upper_ref[:128, :] = upper_ref[:, pl.ds(group, 128)].T
    slab_ref[...] = upper_ref[pl.ds(pl.multiple_of((mine % 16) * 8, 8), 8), :]

    for h in range(2):
        for s in range(1, 4):
            line = cols_ref.at[h, ((d, c)[h] - s + 4) % 4]
            remote(line, line, c_send.at[h, 3 + s], c_recv.at[h, 3 + s], partner).wait_recv()
    for s in range(8):
        slot = rows_ref.at[2 * ((z - s + 8) % 8) + 1 - k]
        remote(slot, slot, rp_send.at[s], rp_recv.at[s], partner).wait_recv()

    @pl.when(jnp.logical_not(fixed))
    def _():
        remote(piece, turned, turn_send, turn_recv, turn_peer).wait_send()

    for copy in sent:
        copy.wait_send()
    keep_turned.wait()
    for step in range(ORDER // 128):
        store_group(step).wait()


def exchange_and_factor(diag_block, panel):
    hbm = pl.BlockSpec(memory_space=pltpu.MemorySpace.HBM)
    dma = pltpu.SemaphoreType.DMA
    return pl.pallas_call(
        exchange_kernel,
        out_shape=(
            jax.ShapeDtypeStruct((2, 4, 4, 128, 128), F32),
            jax.ShapeDtypeStruct((16, 256, 128), F32),
            jax.ShapeDtypeStruct((ORDER, ORDER), F32),
            jax.ShapeDtypeStruct((8, ORDER), F32),
        ),
        in_specs=[hbm, hbm],
        out_specs=(hbm, hbm, hbm, pl.BlockSpec(memory_space=pltpu.VMEM)),
        scratch_shapes=[
            pltpu.VMEM((2, 4, 4, 8, 8, 128), F32),
            pltpu.VMEM((256, 128), F32),
            pltpu.VMEM((256, 128), F32),
            pltpu.VMEM((ORDER, ORDER), F32),
            pltpu.VMEM((ORDER, ORDER), F32),
            pltpu.VMEM((6 * 128, ORDER), BF16),
            dma((3,)),
            dma((3,)),
            dma((8,)),
            dma((8,)),
            dma((2, 15)),
            dma((2, 15)),
            dma((2, 16)),
            dma((2, 16)),
            dma,
            dma,
            dma((9,)),
            dma((9,)),
            dma((8,)),
            dma((8,)),
            dma((2, 7)),
            dma((2, 7)),
            dma((4,)),
        ],
        compiler_params=pltpu.CompilerParams(collective_id=0, has_side_effects=True),
        name="exchange_and_factor",
    )(diag_block, panel)


def split2(x):
    high = x.astype(BF16)
    return high, (x - high.astype(F32)).astype(BF16)


def dot3(left, right, depth_axis):
    (lh, ll), (rh, rl) = left, right
    return lax.dot_general(
        jnp.concatenate([lh, lh, ll], axis=1),
        jnp.concatenate([rh, rl, rh], axis=depth_axis),
        (((1,), (depth_axis,)), ((), ())),
        preferred_element_type=F32,
    )


def update_kernel(
    cols_ref, rows_ref, inv_ref, slab_ref, trail_ref,
    slab_out, panel_out, schur_ref, ih_ref, il_ref, sh_ref, sl_ref,
):
    def cols_piece(q):
        return split2(jnp.concatenate([
            jnp.concatenate([cols_ref[0, e, q], cols_ref[1, q, e]], axis=0) for e in range(4)
        ], axis=1))

    @pl.when(pl.program_id(0) == 0)
    def _():
        slab_out[...] = slab_ref[...]
        ih, il = split2(inv_ref[...])
        for q in range(4):
            ph, pl_ = cols_piece(q)
            top = dot3((ih[:256, :256], il[:256, :256]), (ph[:, :256], pl_[:, :256]), 1)
            low = dot3((ih[256:], il[256:]), (ph, pl_), 1)
            part = slice(256 * q, 256 * q + 256)
            sh_ref[:, part], sl_ref[:, part] = split2(jnp.concatenate([top, low], axis=0))
        ih_ref[...], il_ref[...] = split2(inv_ref[...].T)
        first = pl.multiple_of(lax.axis_index("depth") * 128, 128)
        panel_out[...] = dot3(
            cols_piece(lax.axis_index("col")), split2(inv_ref[pl.ds(first, 128), :]), 1
        )

    ph, pl_ = split2(jnp.concatenate([rows_ref[0, e] for e in range(4)], axis=1))
    left = dot3((ph[:, :256], pl_[:, :256]), (ih_ref[:256, :256], il_ref[:256, :256]), 0)
    right = dot3((ph, pl_), (ih_ref[:, 256:], il_ref[:, 256:]), 0)
    mine = split2(jnp.concatenate([left, right], axis=1))
    schur_ref[...] = trail_ref[...] - dot3(mine, (sh_ref[...], sl_ref[...]), 0)


TILE = 256


def solve_and_update(cols, rows, inverse, slab, trailing):
    def whole(*shape):
        return pl.BlockSpec(shape, lambda i: (0,) * len(shape), pipeline_mode=pl.Buffered(1))

    tile = pl.BlockSpec((TILE, 1024), lambda i: (i, 0))
    return pl.pallas_call(
        update_kernel,
        grid=(1024 // TILE,),
        in_specs=[
            whole(2, 4, 4, 128, 128),
            pl.BlockSpec((1, 4, TILE, 128), lambda i: (i, 0, 0, 0)),
            whole(ORDER, ORDER),
            whole(8, ORDER),
            tile,
        ],
        out_specs=(whole(8, ORDER), whole(256, 128), tile),
        out_shape=(
            jax.ShapeDtypeStruct((8, ORDER), F32),
            jax.ShapeDtypeStruct((256, 128), F32),
            jax.ShapeDtypeStruct((1024, 1024), F32),
        ),
        scratch_shapes=[
            pltpu.VMEM((ORDER, ORDER), BF16),
            pltpu.VMEM((ORDER, ORDER), BF16),
            pltpu.VMEM((ORDER, 1024), BF16),
            pltpu.VMEM((ORDER, 1024), BF16),
        ],
        name="solve_and_update",
    )(cols, rows.reshape(4, 4, TILE, 128), inverse, slab, trailing)


def local(diag_block, panel, trailing):
    cols, rows, inverse, slab = exchange_and_factor(diag_block, panel)
    return solve_and_update(cols, rows, inverse, slab, trailing)


def solution(mesh):
    in_specs = (P(("row", "col"), None), P(("row", "col"), "depth"), P(("col", "depth"), "row"))
    out_specs = (P(("row", "col"), None), P(("row", "col"), "depth"), P(("col", "depth"), "row"))
    return jax.shard_map(local, mesh=mesh, in_specs=in_specs, out_specs=out_specs, check_vma=False)
```
